256 devices in a mesh: gx: 16 (over y, x_lo, core), gy: 16 (over x_hi, z).
Axes of the slice: x: 4 (x_hi: 2, x_lo: 2; x = x_hi * 2 + x_lo), y: 4, z: 8, core: 2. Of those that a mesh axis runs over, the one named last changes fastest.
Arguments:
- cotangent: float32 [3, 32, 32, 128], P(None, 'gx', 'gy'), may hold values from -4 to 4
- polarizability: float32 [32, 32, 128], P('gx', 'gy'), may hold values from 0.2 to 1.6
- site_offset: int32 [3, 32, 32, 128], P(None, 'gx', 'gy'), may hold values from 0 to 15, as said below
- site_fraction: float32 [3, 32, 32, 128], P(None, 'gx', 'gy'), may hold values from 0.2 to 0.8
- cell_count: int32 [32, 32, 16], P('gx', 'gy'), may hold values from 4 to 8, as said below
Outputs:
- adjoint_dipoles: float32 [3, 32, 32, 128], P(None, 'gx', 'gy')
The draws below stay inside these ranges and needn't reach their ends.
Inputs may be any that keep to these rules, and one draw needn't show every extreme that they name: `site_offset`: within a cell the 8 slots name distinct mesh points: no two slots have the same three components. The first component is below 8, the second below 8, the third below 16. `cell_count`: some cell holds 8 live atoms.
All inputs are finite; a program needn't handle non-finite values.
Results may differ from the reference program's by a relative error of at most 0.0001.
Values sent between devices are 32-bit elements; how exact they have to be, the bound alone decides.
A program may use at most 128 MiB of HBM per device.

```python
import math
import jax
import jax.numpy as jnp
from jax import lax

A = 8
NCZ = 16
HX = 8
HY = 8
HZ = 16
ITERS = 2
NCX = 32
NCY = 32
KX = 256
KY = 256
KZ = 256


def draw_cotangent(key, part):
    shape = (3, NCX, NCY, NCZ * A)
    return jnp.clip(jax.random.normal(jax.random.fold_in(key, 43), shape, jnp.float32), -4.0, 4.0)


def draw_site_offset(key, part):
    count = NCX * NCY * NCZ
    keys = jax.random.split(jax.random.fold_in(key, 11), count)

    def pick(one_key):
        return jax.random.permutation(one_key, HX * HY * HZ)[:A]
    chosen = jax.vmap(pick)(keys).astype(jnp.int32).reshape(NCX, NCY, NCZ * A)
    first = chosen // (HY * HZ)
    second = chosen // HZ % HY
    third = chosen % HZ
    return jnp.stack([first, second, third], axis=0)


def draw_cell_count(key, part):
    count = NCX * NCY * NCZ
    base = jax.random.randint(jax.random.fold_in(key, 23), (NCX, NCY, NCZ), A // 2, A + 1, dtype=jnp.int32)
    chosen = jax.random.randint(jax.random.fold_in(key, 29), (), 0, count, dtype=jnp.int32)
    flat = jnp.arange(count, dtype=jnp.int32).reshape(NCX, NCY, NCZ)
    return jnp.where(flat == chosen, A, base).astype(jnp.int32)


def levels(key, extent, cuts, least, high):
    gain = 1.0
    for position, shards_of in cuts:
        heights = jax.random.uniform(jax.random.fold_in(jax.random.fold_in(key, 6), position), (shards_of,), jnp.float32, least / len(cuts), high / len(cuts))
        gain = gain * jnp.repeat(jnp.exp(heights), extent[position] // shards_of).reshape((-1,) + (1,) * (len(extent) - 1 - position))
    return gain


def setup_inputs(seed: int = 0) -> dict:
    key_of = jax.random.split(jax.random.key(seed), 6)
    return {
        "cotangent": draw_cotangent(jax.random.fold_in(key_of[5], 71), 0),
        "polarizability": jnp.clip(jnp.exp(math.log(1.6) - 2.0794415 * jax.random.uniform(key_of[1], (NCX, NCY, NCZ * A), jnp.float32) ** levels(key_of[1], (NCX, NCY, NCZ * A), ((0, 16), (1, 16)), -0.2, 0.2)), 0.2, 1.6),
        "site_offset": draw_site_offset(jax.random.fold_in(key_of[5], 71), 0),
        "site_fraction": jnp.clip(0.2 + 0.6 * jax.random.uniform(key_of[3], (3, NCX, NCY, NCZ * A), jnp.float32) ** levels(key_of[3], (3, NCX, NCY, NCZ * A), ((1, 16), (2, 16)), -0.2, 0.2), 0.2, 0.8),
        "cell_count": draw_cell_count(jax.random.fold_in(key_of[5], 71), 0),
    }


BETA = 0.7
THOLE = 0.39
ROOT_PI = 1.7724538509055159
SELF_GAIN = 4.0 * BETA * BETA * BETA / (3.0 * ROOT_PI)
NEIGHBOUR_SHIFTS = [(a, b, c) for a in (-1, 0, 1) for b in (-1, 0, 1) for c in (-1, 0, 1)]

def coefficients(square, root):
    distance = jnp.sqrt(square)
    inverse_square = 1.0 / square
    screened = jax.scipy.special.erfc(BETA * distance) / distance
    gauss = 2.0 * BETA / ROOT_PI * jnp.exp(-BETA * BETA * square)
    first = (screened + gauss) * inverse_square
    second = (3.0 * first + 2.0 * BETA * BETA * gauss) * inverse_square
    scaled = THOLE * square * distance / root
    damping = jnp.exp(-scaled)
    inverse_cube = inverse_square / distance
    first = first - damping * inverse_cube
    second = second - 3.0 * (1.0 + scaled) * damping * inverse_cube * inverse_square
    return (first, second)

def pair_terms(place_own, polar_own, place_near, polar_near, self_pair):
    separation = place_own[:, :, :, None] - place_near[:, :, None, :]
    square = separation[0] * separation[0] + separation[1] * separation[1] + separation[2] * separation[2]
    square = jnp.where(self_pair, 1.0, square)
    root = jnp.sqrt(polar_own[:, :, None] * polar_near[:, None, :])
    first, second = coefficients(square, root)
    first = jnp.where(self_pair, 0.0, first)
    second = jnp.where(self_pair, 0.0, second)
    return (separation, first, second)

def pair_apply(separation, first, second, moment_near):
    along = moment_near[:, :, None, :]
    projected = lax.optimization_barrier(jnp.sum(separation * along, axis=0))
    return lax.optimization_barrier(jnp.sum(second * projected * separation - first * along, axis=3))

def spline(fraction):
    rest = 1.0 - fraction
    square = fraction * fraction
    cube = square * fraction
    values = jnp.stack([rest * rest * rest / 6.0, (3.0 * cube - 6.0 * square + 4.0) / 6.0, (-3.0 * cube + 3.0 * square + 3.0 * fraction + 1.0) / 6.0, cube / 6.0], axis=-1)
    slopes = jnp.stack([-0.5 * rest * rest, 0.5 * (3.0 * square - 4.0 * fraction), 0.5 * (-3.0 * square + 2.0 * fraction + 1.0), 0.5 * square], axis=-1)
    return (values, slopes)

def neighbour_stack(cells):
    pieces = []
    for across, along, upward in NEIGHBOUR_SHIFTS:
        pieces.append(jnp.roll(cells, (-across, -along, -upward), axis=(1, 2, 3)))
    return jnp.stack(pieces, axis=4)

def by_column(values):
    return jnp.transpose(values, (1, 0, 2, 3, 4)).reshape(NCX, values.shape[0], NCY * NCZ, values.shape[4])

def green_table(dtype):

    def part(length):
        grid = jnp.arange(length, dtype=jnp.int32)
        signed = jnp.where(2 * grid < length, grid, grid - length).astype(dtype) / length
        angle = 2.0 * math.pi / length * grid.astype(dtype)
        factor = 9.0 / ((2.0 + jnp.cos(angle)) * (2.0 + jnp.cos(angle)))
        return (grid, signed * signed, factor)
    grid_x, square_x, factor_x = part(KX)
    grid_y, square_y, factor_y = part(KY)
    grid_z, square_z, factor_z = part(KZ)
    square = square_x[:, None, None] + square_y[None, :, None] + square_z[None, None, :]
    anchor = (grid_x[:, None, None] == 0) & (grid_y[None, :, None] == 0) & (grid_z[None, None, :] == 0)
    safe = jnp.where(anchor, 1.0, square)
    value = jnp.exp(-(math.pi / BETA) * (math.pi / BETA) * safe) / (math.pi * safe)
    value = value * factor_x[:, None, None] * factor_y[None, :, None] * factor_z[None, None, :]
    return jnp.where(anchor, 0.0, value)

def reference(cotangent, polarizability, site_offset, site_fraction, cell_count):
    dtype = cotangent.dtype
    slot = jnp.arange(A, dtype=jnp.int32)
    live = (slot < cell_count[..., None]).astype(dtype).reshape(NCX, NCY, NCZ * A)
    place = site_offset.astype(dtype) + 1.0 + site_fraction
    shifts = jnp.asarray(NEIGHBOUR_SHIFTS, dtype=dtype).T * jnp.asarray([HX, HY, HZ], dtype=dtype)[:, None]
    place_cells = place.reshape(3, NCX, NCY, NCZ, A)
    polar_cells = polarizability.reshape(1, NCX, NCY, NCZ, A)
    moved = neighbour_stack(place_cells) + shifts[:, None, None, None, :, None]
    place_near = by_column(moved.reshape(3, NCX, NCY, NCZ, 27 * A))
    polar_near = by_column(neighbour_stack(polar_cells).reshape(1, NCX, NCY, NCZ, 27 * A))[:, 0]
    place_own = by_column(place_cells)
    polar_own = by_column(polar_cells)[:, 0]
    index = jnp.arange(27 * A, dtype=jnp.int32)
    self_pair = (index[None, :] // A == 13) & (index[None, :] % A == slot[:, None])

    def column_field(item):
        separation, first, second = pair_terms(item[0], item[1], item[2], item[3], self_pair)
        return pair_apply(separation, first, second, item[4])

    def near_field(moment):
        cells = moment.reshape(3, NCX, NCY, NCZ, A)
        moment_near = by_column(neighbour_stack(cells).reshape(3, NCX, NCY, NCZ, 27 * A))
        blocks = lax.map(column_field, (place_own, polar_own, place_near, polar_near, moment_near))
        return jnp.transpose(blocks, (1, 0, 2, 3)).reshape(3, NCX, NCY, NCZ * A)
    cell_x = jnp.arange(NCX, dtype=jnp.int32)[:, None, None]
    cell_y = jnp.arange(NCY, dtype=jnp.int32)[None, :, None]
    cell_z = (jnp.arange(NCZ * A, dtype=jnp.int32) // A)[None, None, :]
    corner = jnp.arange(4, dtype=jnp.int32)
    grid_x = ((cell_x * HX + site_offset[0]).reshape(-1)[:, None] + corner) % KX
    grid_y = ((cell_y * HY + site_offset[1]).reshape(-1)[:, None] + corner) % KY
    grid_z = ((cell_z * HZ + site_offset[2]).reshape(-1)[:, None] + corner) % KZ
    values_x, slopes_x = spline(site_fraction[0].reshape(-1))
    values_y, slopes_y = spline(site_fraction[1].reshape(-1))
    values_z, slopes_z = spline(site_fraction[2].reshape(-1))
    gather_index = (grid_x[:, :, None, None], grid_y[:, None, :, None], grid_z[:, None, None, :])
    slope_first = slopes_x[:, :, None, None] * values_y[:, None, :, None] * values_z[:, None, None, :]
    slope_second = values_x[:, :, None, None] * slopes_y[:, None, :, None] * values_z[:, None, None, :]
    slope_third = values_x[:, :, None, None] * values_y[:, None, :, None] * slopes_z[:, None, None, :]
    green = green_table(dtype)

    def far_field(moment):
        flat = moment.reshape(3, -1)
        weight = flat[0][:, None, None, None] * slope_first + flat[1][:, None, None, None] * slope_second + flat[2][:, None, None, None] * slope_third
        charge = jnp.zeros((KX, KY, KZ), dtype).at[gather_index].add(weight)
        potential = jnp.real(jnp.fft.ifftn(green * jnp.fft.fftn(charge))).astype(dtype)
        sampled = potential[gather_index]
        field = jnp.stack([-lax.optimization_barrier(jnp.sum(slope_first * sampled, axis=(1, 2, 3))), -lax.optimization_barrier(jnp.sum(slope_second * sampled, axis=(1, 2, 3))), -lax.optimization_barrier(jnp.sum(slope_third * sampled, axis=(1, 2, 3)))], axis=0)
        return field.reshape(3, NCX, NCY, NCZ * A)
    moment = live * polarizability * cotangent
    for turn in range(ITERS):
        field = near_field(moment) + far_field(moment) + SELF_GAIN * moment
        moment = live * polarizability * (cotangent + field)
    return moment
```

```python
import math

import jax
import jax.numpy as jnp
import ml_dtypes
import numpy as np
from jax import lax
from jax.experimental import pallas as pl
from jax.experimental.pallas import tpu as pltpu
from jax.sharding import PartitionSpec as P

BETA = 0.7
THOLE = 0.39
ROOT_PI = 1.7724538509055159
SELF_GAIN = 4.0 * BETA * BETA * BETA / (3.0 * ROOT_PI)
ITERS = 2
N = 256
SIDE = 16
MESH = pl.DeviceIdType.MESH
F32 = jnp.float32
BF16 = jnp.bfloat16

ERFC_P = (
    2.326819970068386e-2,
    -1.387039388740657e-1,
    3.687424674597105e-1,
    -5.824733027278666e-1,
    6.210004621745983e-1,
    -4.944515323274145e-1,
    3.404879937665872e-1,
    -2.741127028184656e-1,
    5.638259427386472e-1,
)
ERFC_R = (
    -1.047766399936249e1,
    1.297719955372516e1,
    -7.495518717768503e0,
    2.921019019210786e0,
    -1.015265279202700e0,
    4.218463358204948e-1,
    -2.820767439740514e-1,
    5.641895067754075e-1,
)
ERF_T = (
    7.853861353153693e-5,
    -8.010193625184903e-4,
    5.188327685732524e-3,
    -2.685381193529856e-2,
    1.128358514861418e-1,
    -3.761262582423300e-1,
    1.128379165726710e0,
)


def halves_np(table):
    high = table.astype(np.float32).astype(ml_dtypes.bfloat16)
    low = (table - high.astype(np.float64)).astype(np.float32).astype(ml_dtypes.bfloat16)
    return high, low


def tables():
    grid = np.arange(N)
    angle = 2.0 * math.pi / N * (grid[:, None] * grid[None, :] % N)
    hartley = np.cos(angle) + np.sin(angle)
    short = np.arange(SIDE)
    pair = (
        short[:, None, None, None] * short[None, None, :, None]
        + short[None, :, None, None] * short[None, None, None, :]
    ).reshape(N, N)
    outer = 2.0 * math.pi / SIDE * (pair % SIDE)
    twist = 2.0 * math.pi / N * (pair % N)

    def part(freq):
        signed = np.where(2 * freq < N, freq, freq - N) / N
        factor = 9.0 / (2.0 + np.cos(2.0 * math.pi * freq / N)) ** 2
        return signed * signed, factor

    low_x = short[:, None, None, None]
    low_y = short[None, :, None, None]
    freq_x = (low_x + SIDE * short[None, None, :, None]) + 0 * low_y
    freq_y = (low_y + SIDE * short[None, None, None, :]) + 0 * low_x
    square_x, factor_x = part(freq_x)
    square_y, factor_y = part(freq_y)
    square = (square_x + square_y).reshape(N, N)
    gain = (
        np.exp(-((math.pi / BETA) ** 2) * (square_x + square_y)) * factor_x * factor_y / math.pi
    ).reshape(N, N) / float(N * N * N)
    return (
        *halves_np(hartley),
        *halves_np(np.cos(outer)),
        *halves_np(-np.sin(outer)),
        np.cos(twist).astype(np.float32),
        (-np.sin(twist)).astype(np.float32),
        gain.astype(np.float32),
        square.astype(np.float32),
    )


TABLES = tables()

NN = (((1,), (0,)), ((), ()))
NT = (((1,), (1,)), ((), ()))


def halves(value):
    high = value.astype(BF16)
    return high, (value - high.astype(F32)).astype(BF16)


def product(left, right, dims=NN):
    def dot(a, b):
        return lax.dot_general(a, b, dims, preferred_element_type=F32)

    return dot(left[0], right[0]) + (dot(left[0], right[1]) + dot(left[1], right[0]))


def polynomial(terms, value):
    total = jnp.full_like(value, terms[0])
    for term in terms[1:]:
        total = total * value + term
    return total


def pair_coefficients(square, root):
    inverse = lax.rsqrt(square)
    distance = square * inverse
    inverse_square = 1.0 / square
    argument = BETA * distance
    steep = argument * argument
    bell = jnp.exp(-steep)
    ratio = inverse * (1.0 / BETA)
    small = ratio * ratio
    tail = jnp.where(
        argument < 2.0, polynomial(ERFC_P, small), polynomial(ERFC_R, small)
    )
    erfc = jnp.where(
        argument < 1.0,
        1.0 - argument * polynomial(ERF_T, steep),
        bell * ratio * tail,
    )
    gauss = (2.0 * BETA / ROOT_PI) * bell
    first = (erfc * inverse + gauss) * inverse_square
    second = (3.0 * first + (2.0 * BETA * BETA) * gauss) * inverse_square
    scaled = THOLE * square * distance * root
    damping = jnp.exp(-scaled)
    inverse_cube = inverse_square * inverse
    first = first - damping * inverse_cube
    second = second - 3.0 * (1.0 + scaled) * damping * inverse_cube * inverse_square
    return first, second


def spline(f):
    rest = 1.0 - f
    square = f * f
    cube = square * f
    values = (
        rest * rest * rest / 6.0,
        (3.0 * cube - 6.0 * square + 4.0) / 6.0,
        (-3.0 * cube + 3.0 * square + 3.0 * f + 1.0) / 6.0,
        cube / 6.0,
    )
    slopes = (
        -0.5 * rest * rest,
        0.5 * (3.0 * square - 4.0 * f),
        0.5 * (-3.0 * square + 2.0 * f + 1.0),
        0.5 * square,
    )
    return values, slopes


def placed(place, weights):
    total = jnp.where(place == 0, weights[0], 0.0)
    for order in range(1, 4):
        total = jnp.where(place == order, weights[order], total)
    return total


def kernel(
    cot, pol, off, frac, cnt, h_hi, h_lo, c_hi, c_lo, s_hi, s_lo, t_re, t_im, gain, square_xy,
    out,
    fixed, moving, own, prod, wz_hi, wz_lo, p_hi, p_lo, spread, send_a, send_b, land_a, land_b,
    near_static, near_moving, tensor, near, far, far_in,
    send_s, recv_s, halo_send, halo_recv, part_send, part_recv, second_level,
):
    mx = lax.axis_index("gx")
    my = lax.axis_index("gy")
    me = mx * SIDE + my

    def wrap(i):
        return lax.rem(i + SIDE, SIDE)

    entry = pltpu.get_barrier_semaphore()

    def greet(i, carry):
        pl.semaphore_signal(entry, inc=1, device_id=(wrap(mx + i), my), device_id_type=MESH)
        pl.semaphore_signal(entry, inc=1, device_id=(mx, wrap(my + i)), device_id_type=MESH)
        return carry

    lax.fori_loop(1, SIDE, greet, 0)
    for a in (-1, 1):
        for b in (-1, 1):
            pl.semaphore_signal(
                entry, inc=1, device_id=(wrap(mx + a), wrap(my + b)), device_id_type=MESH
            )

    lane = lax.broadcasted_iota(jnp.int32, (8, 128), 1)
    row = lax.broadcasted_iota(jnp.int32, (8, 128), 0)
    expand = (
        lax.broadcasted_iota(jnp.int32, (16, 128), 1) // 8
        == lax.broadcasted_iota(jnp.int32, (16, 128), 0)
    ).astype(F32)
    slot = (lax.broadcasted_iota(jnp.int32, (2, 128), 1) % 8).astype(F32)
    for cx in range(2):
        counts = jnp.dot(cnt[cx].astype(F32), expand, preferred_element_type=F32)
        weight = jnp.where(slot < counts, 1.0, 0.0) * pol[cx]
        for cy in range(2):
            w = weight[cy : cy + 1]
            c3 = [cot[c, cx, cy : cy + 1] for c in range(3)]
            zero = jnp.zeros((1, 128), F32)
            fixed[cx + 1, cy + 1] = jnp.concatenate(
                [off[c, cx, cy : cy + 1].astype(F32) for c in range(3)]
                + [frac[c, cx, cy : cy + 1] for c in range(3)]
                + [pol[cx, cy : cy + 1], zero],
                axis=0,
            )
            own[cx, cy] = jnp.concatenate(c3 + [w, zero, zero, zero, zero], axis=0)
            moving[0, cx + 1, cy + 1] = jnp.concatenate(
                [w * c3[c] for c in range(3)] + [zero] * 5, axis=0
            )

    pl.semaphore_wait(entry, 2 * (SIDE - 1) + 4)

    def second(i, carry):
        pl.semaphore_signal(
            second_level, inc=1, device_id=(wrap(mx + i), my), device_id_type=MESH
        )
        return carry

    lax.fori_loop(1, SIDE, second, 0)

    def halo(ref, slot_of):
        copies = []
        k = 0
        for a in (-1, 0, 1):
            for b in (-1, 0, 1):
                if a == 0 and b == 0:
                    continue
                src_x = {-1: pl.ds(1, 1), 0: pl.ds(1, 2), 1: pl.ds(2, 1)}[a]
                src_y = {-1: pl.ds(1, 1), 0: pl.ds(1, 2), 1: pl.ds(2, 1)}[b]
                dst_x = {-1: pl.ds(3, 1), 0: pl.ds(1, 2), 1: pl.ds(0, 1)}[a]
                dst_y = {-1: pl.ds(3, 1), 0: pl.ds(1, 2), 1: pl.ds(0, 1)}[b]
                copies.append(
                    pltpu.make_async_remote_copy(
                        src_ref=ref.at[src_x, src_y],
                        dst_ref=ref.at[dst_x, dst_y],
                        send_sem=halo_send.at[slot_of, k],
                        recv_sem=halo_recv.at[slot_of, k],
                        device_id=(wrap(mx + a), wrap(my + b)),
                        device_id_type=MESH,
                    )
                )
                k += 1
        return copies

    first_halo = halo(fixed, 2) + halo(moving.at[0], 0)
    for copy in first_halo:
        copy.start()
    for copy in first_halo:
        copy.wait()

    pick = [((lane // 8 + dz + 16) % 16) * 8 + row for dz in (-1, 0, 1)]

    def expanded(line, k):
        return jnp.take_along_axis(
            jnp.broadcast_to(line, (8, 128)), pick[k], axis=1, mode="promise_in_bounds"
        )

    def grow_static(col, carry):
        tile = fixed[col // 4, lax.rem(col, 4)]
        lines = [tile[c : c + 1] + 1.0 + tile[c + 3 : c + 4] for c in range(3)] + [tile[6:7]]
        for k in range(3):
            for c in range(4):
                value = expanded(lines[c], k)
                if c == 2:
                    value = value + 16.0 * (k - 1)
                near_static[col, k, c] = value
        return carry

    def grow_moving(it):
        def body(col, carry):
            tile = moving[it, col // 4, lax.rem(col, 4)]
            for k in range(3):
                for c in range(3):
                    near_moving[col, k, c] = expanded(tile[c : c + 1], k)
            return carry

        lax.fori_loop(0, 16, body, 0)

    tall = lax.broadcasted_iota(jnp.int32, (N, 128), 0)
    low = lax.broadcasted_iota(jnp.int32, (SIDE, 128), 0)
    cell_z = lax.broadcasted_iota(jnp.int32, (1, 128), 1) // 8 * 16

    def weights(col, carry):
        ex = col // 3
        ey = lax.rem(col, 3)
        tile = fixed[ex, ey]
        anchor = tile[0:3].astype(jnp.int32)
        value, slope = zip(*[spline(tile[c + 3 : c + 4]) for c in range(3)])
        place_x = low - (anchor[0:1] + (ex - 1) * 8)
        place_y = low - (anchor[1:2] + (ey - 1) * 8)
        place_z = (tall - (anchor[2:3] + cell_z)) & (N - 1)
        wx, sx = placed(place_x, value[0]), placed(place_x, slope[0])
        wy, sy = placed(place_y, value[1]), placed(place_y, slope[1])
        for x in range(SIDE):
            rows = pl.ds(x * SIDE, SIDE)
            prod[col, 0, rows] = sx[x : x + 1] * wy
            prod[col, 1, rows] = wx[x : x + 1] * sy
            prod[col, 2, rows] = wx[x : x + 1] * wy
        for k, source in enumerate((value[2], slope[2])):
            high, rest = halves(placed(place_z, source))
            wz_hi[col, :, pl.ds(128 * k, 128)] = high
            wz_lo[col, :, pl.ds(128 * k, 128)] = rest
        return carry

    lax.fori_loop(0, 9, weights, 0)

    def pairs(item, carry):
        q = item // 9
        nb = lax.rem(item, 9)
        cx = q // 2
        cy = lax.rem(q, 2)
        dx = nb // 3 - 1
        dy = lax.rem(nb, 3) - 1
        tile = fixed[cx + 1, cy + 1]
        here = [tile[c : c + 1] + 1.0 + tile[c + 3 : c + 4] for c in range(3)]
        here[0] = here[0] - (8 * dx).astype(F32)
        here[1] = here[1] - (8 * dy).astype(F32)
        mine = tile[6:7]
        col = (cx + 1 + dx) * 4 + cy + 1 + dy
        for k in range(3):
            apart = [here[c] - near_static[col, k, c] for c in range(3)]
            square = apart[0] * apart[0] + apart[1] * apart[1] + apart[2] * apart[2]
            root = lax.rsqrt(mine * near_static[col, k, 3])
            if k == 1:
                same = (row == lane % 8) & (nb == 4)
                square = jnp.where(same, 1.0, square)
            c1, c2 = pair_coefficients(square, root)
            if k == 1:
                c1 = jnp.where(same, 0.0, c1)
                c2 = jnp.where(same, 0.0, c2)
            scaled = [c2 * apart[c] for c in range(3)]
            tensor[item, k, 0] = scaled[0] * apart[0] - c1
            tensor[item, k, 1] = scaled[1] * apart[1] - c1
            tensor[item, k, 2] = scaled[2] * apart[2] - c1
            tensor[item, k, 3] = scaled[0] * apart[1]
            tensor[item, k, 4] = scaled[0] * apart[2]
            tensor[item, k, 5] = scaled[1] * apart[2]
        return carry

    def near_field(it):
        grow_moving(it)

        def body(q, carry):
            cx = q // 2
            cy = lax.rem(q, 2)

            def inner(nb, total):
                fx, fy, fz = total
                col = (cx + nb // 3) * 4 + cy + lax.rem(nb, 3)
                item = q * 9 + nb
                for k in range(3):
                    vx, vy, vz = [near_moving[col, k, c] for c in range(3)]
                    xx, yy, zz, xy, xz, yz = [tensor[item, k, c] for c in range(6)]
                    fx = fx + (xx * vx + xy * vy + xz * vz)
                    fy = fy + (xy * vx + yy * vy + yz * vz)
                    fz = fz + (xz * vx + yz * vy + zz * vz)
                return fx, fy, fz

            zero = jnp.zeros((8, 128), F32)
            sums = lax.fori_loop(0, 9, inner, (zero, zero, zero))
            near[q] = jnp.concatenate(
                [jnp.sum(s, axis=0, keepdims=True) for s in sums]
                + [jnp.zeros((5, 128), F32)],
                axis=0,
            )
            return carry

        lax.fori_loop(0, 4, body, 0)

    def exchange(source, target, k):
        def copy(t):
            return pltpu.make_async_remote_copy(
                src_ref=source.at[t],
                dst_ref=target.at[me],
                send_sem=send_s.at[k],
                recv_sem=recv_s.at[k],
                device_id=(t // SIDE, lax.rem(t, SIDE)),
                device_id_type=MESH,
            )

        def send(i, carry):
            copy(lax.rem(me + i, N)).start()
            return carry

        lax.fori_loop(1, N, send, 0)
        target[me] = source[me]

    def arrive(source, target, k):
        pltpu.make_async_remote_copy(
            src_ref=source.at[pl.ds(0, N - 1)],
            dst_ref=target.at[pl.ds(0, N - 1)],
            send_sem=send_s.at[k],
            recv_sem=recv_s.at[k],
            device_id=(mx, wrap(my + 1)),
            device_id_type=MESH,
        ).wait()

    hartley = (h_hi, h_lo)

    def loaded(pair):
        return pair[0][...], pair[1][...]

    def put_rows(ref, value):
        ref[:, 0, :] = value[:, :128]
        ref[:, 1, :] = value[:, 128:]

    def get_rows(ref):
        return jnp.concatenate([ref[:, 0, :], ref[:, 1, :]], axis=1)

    def filtered(value):
        cosine = (c_hi[...], c_lo[...])
        sine = (s_hi[...], s_lo[...])
        parts = halves(value)
        re = product(cosine, parts)
        im = product(sine, parts)
        tr, ti = t_re[...], t_im[...]
        first = halves(re * tr - im * ti)
        other = halves(re * ti + im * tr)
        re = product(first, cosine) - product(other, sine)
        im = product(first, sine) + product(other, cosine)
        line = jnp.zeros((1, 128), F32) + me.astype(F32)
        signed = jnp.where(line < N // 2, line, line - N) * (1.0 / N)
        height = signed * signed
        bend = 2.0 + jnp.cos(line * (2.0 * math.pi / N))
        strength = jnp.exp(-((math.pi / BETA) ** 2) * height) * 9.0 / (bend * bend)
        height = jnp.concatenate([height, height], axis=1)
        strength = jnp.concatenate([strength, strength], axis=1)
        square = square_xy[...] + height
        centre = square == 0.0
        green = jnp.where(
            centre, 0.0, gain[...] * strength / jnp.where(centre, 1.0, square)
        )
        first = halves(re * green)
        other = halves(im * green)
        re = product(first, cosine) + product(other, sine)
        im = product(other, cosine) - product(first, sine)
        first = halves(re * tr + im * ti)
        other = halves(im * tr - re * ti)
        return product(cosine, first) + product(sine, other)

    def iteration(it, carry):
        def rows(col, carry):
            tile = moving[it, col // 3, lax.rem(col, 3)]
            plain = tile[0:1] * prod[col, 0] + tile[1:2] * prod[col, 1]
            steep = tile[2:3] * prod[col, 2]
            lanes = pl.ds(pl.multiple_of(col * N, N), 128)
            lanes_2 = pl.ds(pl.multiple_of(col * N + 128, 128), 128)
            p_hi[:, lanes], p_lo[:, lanes] = halves(plain)
            p_hi[:, lanes_2], p_lo[:, lanes_2] = halves(steep)
            return carry

        lax.fori_loop(0, 9, rows, 0)
        spread[...] = jnp.zeros((N, N), F32)

        def accumulate(col, carry):
            lanes = pl.ds(pl.multiple_of(col * N, N), N)
            spread[...] += product(
                (wz_hi[col], wz_lo[col]), (p_hi[:, lanes], p_lo[:, lanes]), NT
            )
            return carry

        lax.fori_loop(0, 9, accumulate, 0)
        put_rows(send_a, product(loaded(hartley), halves(spread[...])))

        @pl.when(it == 0)
        def _():
            pl.semaphore_wait(second_level, SIDE - 1)

        exchange(send_a, land_a.at[it], 2 * it)

        @pl.when(it == 0)
        def _():
            lax.fori_loop(0, 16, grow_static, 0)
            lax.fori_loop(0, 36, pairs, 0)

        arrive(send_a, land_a.at[it], 2 * it)
        put_rows(send_b, filtered(get_rows(land_a.at[it])))
        exchange(send_b, land_b.at[it], 2 * it + 1)
        near_field(it)
        arrive(send_b, land_b.at[it], 2 * it + 1)
        potential = product(loaded(hartley), halves(get_rows(land_b.at[it])))
        spread[...] = potential.T

        def gather(col, carry):
            sampled = product(halves(spread[...]), (wz_hi[col], wz_lo[col]))
            plain = sampled[:, :128]
            steep = sampled[:, 128:]
            far[col // 3, lax.rem(col, 3)] = jnp.concatenate(
                [
                    jnp.sum(prod[col, 0] * plain, axis=0, keepdims=True),
                    jnp.sum(prod[col, 1] * plain, axis=0, keepdims=True),
                    jnp.sum(prod[col, 2] * steep, axis=0, keepdims=True),
                    jnp.zeros((5, 128), F32),
                ],
                axis=0,
            )
            return carry

        lax.fori_loop(0, 9, gather, 0)
        copies = []
        for k, (a, b) in enumerate(((1, 0), (0, 1), (1, 1))):
            span_x = pl.ds(0, 1) if a else pl.ds(1, 2)
            span_y = pl.ds(0, 1) if b else pl.ds(1, 2)
            land_x = pl.ds(0, 1) if a else pl.ds(0, 2)
            land_y = pl.ds(0, 1) if b else pl.ds(0, 2)
            copies.append(
                pltpu.make_async_remote_copy(
                    src_ref=far.at[span_x, span_y],
                    dst_ref=far_in.at[it, k, land_x, land_y],
                    send_sem=part_send.at[it, k],
                    recv_sem=part_recv.at[it, k],
                    device_id=(wrap(mx - a), wrap(my - b)),
                    device_id_type=MESH,
                )
            )
        for copy in copies:
            copy.start()
        for copy in copies:
            copy.wait()
        for cx in range(2):
            for cy in range(2):
                total = far[cx + 1, cy + 1]
                if cx == 1:
                    total = total + far_in[it, 0, 0, cy]
                if cy == 1:
                    total = total + far_in[it, 1, cx, 0]
                if cx == 1 and cy == 1:
                    total = total + far_in[it, 2, 0, 0]
                field = (
                    near[2 * cx + cy] - total + SELF_GAIN * moving[it, cx + 1, cy + 1]
                )
                tile = own[cx, cy]
                result = tile[3:4] * (tile + field)
                moving[it + 1, cx + 1, cy + 1] = result
                for c in range(3):
                    out[c, cx, cy : cy + 1] = result[c : c + 1]

        @pl.when(it == 0)
        def _():
            copies = halo(moving.at[1], 1)
            for copy in copies:
                copy.start()
            for copy in copies:
                copy.wait()

        return carry

    lax.fori_loop(0, ITERS, iteration, 0)


def shards(cotangent, polarizability, site_offset, site_fraction, cell_count):
    vmem = pl.BlockSpec(memory_space=pltpu.VMEM)

    def room(*shape, dtype=F32):
        return pltpu.VMEM(shape, dtype)

    dma = pltpu.SemaphoreType.DMA
    return pl.pallas_call(
        kernel,
        out_shape=jax.ShapeDtypeStruct((3, 2, 2, 128), F32),
        in_specs=[vmem] * (5 + len(TABLES)),
        out_specs=vmem,
        scratch_shapes=[
            room(4, 4, 8, 128),
            room(3, 4, 4, 8, 128),
            room(2, 2, 8, 128),
            room(9, 3, N, 128),
            room(9, N, N, dtype=BF16),
            room(9, N, N, dtype=BF16),
            room(N, 9 * N, dtype=BF16),
            room(N, 9 * N, dtype=BF16),
            room(N, N),
            room(N, 2, 128),
            room(N, 2, 128),
            room(2, N, 2, 128),
            room(2, N, 2, 128),
            room(16, 3, 4, 8, 128),
            room(16, 3, 3, 8, 128),
            room(36, 3, 6, 8, 128),
            room(4, 8, 128),
            room(3, 3, 8, 128),
            room(2, 3, 2, 2, 8, 128),
            dma((4,)),
            dma((4,)),
            dma((3, 8)),
            dma((3, 8)),
            dma((2, 3)),
            dma((2, 3)),
            pltpu.SemaphoreType.REGULAR,
        ],
        compiler_params=pltpu.CompilerParams(
            collective_id=0, has_side_effects=True, vmem_limit_bytes=56 * 1024 * 1024
        ),
    )(
        cotangent,
        polarizability,
        site_offset,
        site_fraction,
        cell_count,
        *[jnp.asarray(table) for table in TABLES],
    )


def solution(mesh):
    return jax.shard_map(
        shards,
        mesh=mesh,
        in_specs=(
            P(None, "gx", "gy", None),
            P("gx", "gy", None),
            P(None, "gx", "gy", None),
            P(None, "gx", "gy", None),
            P("gx", "gy", None),
        ),
        out_specs=P(None, "gx", "gy", None),
        check_vma=False,
    )
```

```python
import math

import jax
import jax.numpy as jnp
import ml_dtypes
import numpy as np
from jax import lax
from jax.experimental import pallas as pl
from jax.experimental.pallas import tpu as pltpu
from jax.sharding import PartitionSpec as P

BETA = 0.7
THOLE = 0.39
ROOT_PI = 1.7724538509055159
SELF_GAIN = 4.0 * BETA * BETA * BETA / (3.0 * ROOT_PI)
ITERS = 2
N = 256
SIDE = 16
HALF = SIDE * (SIDE // 2 + 1)
MESH = pl.DeviceIdType.MESH
F32 = jnp.float32
BF16 = jnp.bfloat16

ERFC_P = (
    2.326819970068386e-2,
    -1.387039388740657e-1,
    3.687424674597105e-1,
    -5.824733027278666e-1,
    6.210004621745983e-1,
    -4.944515323274145e-1,
    3.404879937665872e-1,
    -2.741127028184656e-1,
    5.638259427386472e-1,
)
ERFC_R = (
    -1.047766399936249e1,
    1.297719955372516e1,
    -7.495518717768503e0,
    2.921019019210786e0,
    -1.015265279202700e0,
    4.218463358204948e-1,
    -2.820767439740514e-1,
    5.641895067754075e-1,
)
ERF_T = (
    7.853861353153693e-5,
    -8.010193625184903e-4,
    5.188327685732524e-3,
    -2.685381193529856e-2,
    1.128358514861418e-1,
    -3.761262582423300e-1,
    1.128379165726710e0,
)


def halves_np(table):
    high = table.astype(np.float32).astype(ml_dtypes.bfloat16)
    low = (table - high.astype(np.float64)).astype(np.float32).astype(ml_dtypes.bfloat16)
    return high, low


def tables():
    grid = np.arange(N)
    angle = 2.0 * math.pi / N * (grid[:, None] * grid[None, :] % N)
    hartley = np.cos(angle) + np.sin(angle)
    short = np.arange(SIDE)
    pair = (
        short[:, None, None, None] * short[None, None, :, None]
        + short[None, :, None, None] * short[None, None, None, :]
    ).reshape(N, N)
    outer = 2.0 * math.pi / SIDE * (pair % SIDE)
    twist = 2.0 * math.pi / N * (pair % N)

    def part(freq):
        signed = np.where(2 * freq < N, freq, freq - N) / N
        factor = 9.0 / (2.0 + np.cos(2.0 * math.pi * freq / N)) ** 2
        return signed * signed, factor

    low_x = short[:, None, None, None]
    low_y = short[None, :, None, None]
    freq_x = (low_x + SIDE * short[None, None, :, None]) + 0 * low_y
    freq_y = (low_y + SIDE * short[None, None, None, :]) + 0 * low_x
    square_x, factor_x = part(freq_x)
    square_y, factor_y = part(freq_y)
    square = (square_x + square_y).reshape(N, N)
    gain = (
        np.exp(-((math.pi / BETA) ** 2) * (square_x + square_y)) * factor_x * factor_y / math.pi
    ).reshape(N, N) / float(N * N * N)
    twice = np.where((grid // SIDE == 0) | (grid // SIDE == SIDE // 2), 1.0, 2.0)
    gain = gain * twice[:, None]
    waves = np.stack(halves_np(np.concatenate([hartley, np.cos(outer), -np.sin(outer)], axis=0)))
    plane = np.stack([np.cos(twist), -np.sin(twist), gain, square])[:, :HALF].astype(np.float32)
    return waves, plane


TABLES = tables()

NN = (((1,), (0,)), ((), ()))
NT = (((1,), (1,)), ((), ()))


def halves(value):
    high = value.astype(BF16)
    return high, (value - high.astype(F32)).astype(BF16)


def product(left, right, dims=NN):
    def dot(a, b):
        return lax.dot_general(a, b, dims, preferred_element_type=F32)

    count = left[0].shape[0]
    both = dot(jnp.concatenate(left, axis=0), right[0])
    return both[:count] + (both[count:] + dot(left[0], right[1]))


def polynomial(terms, value):
    total = jnp.full_like(value, terms[0])
    for term in terms[1:]:
        total = total * value + term
    return total


def pair_coefficients(square, root):
    inverse = lax.rsqrt(square)
    distance = square * inverse
    inverse_square = 1.0 / square
    argument = BETA * distance
    steep = argument * argument
    bell = jnp.exp(-steep)
    ratio = inverse * (1.0 / BETA)
    small = ratio * ratio
    tail = jnp.where(
        argument < 2.0, polynomial(ERFC_P, small), polynomial(ERFC_R, small)
    )
    erfc = jnp.where(
        argument < 1.0,
        1.0 - argument * polynomial(ERF_T, steep),
        bell * ratio * tail,
    )
    gauss = (2.0 * BETA / ROOT_PI) * bell
    first = (erfc * inverse + gauss) * inverse_square
    second = (3.0 * first + (2.0 * BETA * BETA) * gauss) * inverse_square
    scaled = THOLE * square * distance * root
    damping = jnp.exp(-scaled)
    inverse_cube = inverse_square * inverse
    first = first - damping * inverse_cube
    second = second - 3.0 * (1.0 + scaled) * damping * inverse_cube * inverse_square
    return first, second


def spline(f):
    rest = 1.0 - f
    square = f * f
    cube = square * f
    values = (
        rest * rest * rest / 6.0,
        (3.0 * cube - 6.0 * square + 4.0) / 6.0,
        (-3.0 * cube + 3.0 * square + 3.0 * f + 1.0) / 6.0,
        cube / 6.0,
    )
    slopes = (
        -0.5 * rest * rest,
        0.5 * (3.0 * square - 4.0 * f),
        0.5 * (-3.0 * square + 2.0 * f + 1.0),
        0.5 * square,
    )
    return values, slopes


def placed(place, weights):
    total = jnp.where(place == 0, weights[0], 0.0)
    for order in range(1, 4):
        total = jnp.where(place == order, weights[order], total)
    return total


def kernel(
    cot, pol, off, frac, cnt, waves_far, plane_far,
    out,
    waves, plane, fixed, moving, prod, wz_hi, wz_lo, wt_hi, wt_lo, p_hi, p_lo, spread,
    send_a, send_b, land_a, land_b, near_static, near_moving, tensor, near, part, inbox, last_in,
    table_sem, send_s, recv_s, halo_send, halo_recv, part_send, part_recv, second_level,
):
    mx = lax.axis_index("gx")
    my = lax.axis_index("gy")
    me = mx * SIDE + my

    def wrap(i):
        return lax.rem(i + SIDE, SIDE)

    entry = pltpu.get_barrier_semaphore()

    def greet(i, carry):
        pl.semaphore_signal(entry, inc=1, device_id=(wrap(mx + i), my), device_id_type=MESH)
        pl.semaphore_signal(entry, inc=1, device_id=(mx, wrap(my + i)), device_id_type=MESH)
        return carry

    lax.fori_loop(1, SIDE, greet, 0)
    for a in (-1, 1):
        for b in (-1, 1):
            pl.semaphore_signal(
                entry, inc=1, device_id=(wrap(mx + a), wrap(my + b)), device_id_type=MESH
            )

    table_copies = [
        pltpu.make_async_copy(waves_far, waves, table_sem.at[0]),
        pltpu.make_async_copy(plane_far, plane, table_sem.at[1]),
    ]
    for copy in table_copies:
        copy.start()

    lane = lax.broadcasted_iota(jnp.int32, (8, 128), 1)
    row = lax.broadcasted_iota(jnp.int32, (8, 128), 0)
    expand = (
        lax.broadcasted_iota(jnp.int32, (16, 128), 1) // 8
        == lax.broadcasted_iota(jnp.int32, (16, 128), 0)
    ).astype(F32)
    slot = (lax.broadcasted_iota(jnp.int32, (2, 128), 1) % 8).astype(F32)
    for cx in range(2):
        counts = jnp.dot(cnt[cx].astype(F32), expand, preferred_element_type=F32)
        weight = jnp.where(slot < counts, 1.0, 0.0) * pol[cx]
        for cy in range(2):
            here = slice(cy, cy + 1)
            fixed[cx + 1, cy + 1] = jnp.concatenate(
                [off[c, cx, here].astype(F32) for c in range(3)]
                + [frac[c, cx, here] for c in range(3)]
                + [pol[cx, here], weight[here]]
                + [cot[c, cx, here] for c in range(3)]
                + [jnp.zeros((5, 128), F32)],
                axis=0,
            )

    pl.semaphore_wait(entry, 2 * (SIDE - 1) + 4)

    def second(i, carry):
        pl.semaphore_signal(
            second_level, inc=1, device_id=(wrap(mx + i), my), device_id_type=MESH
        )
        return carry

    sides = [(a, b) for a in (-1, 0, 1) for b in (-1, 0, 1) if (a, b) != (0, 0)]

    def spans(table, a, b):
        return tuple(pl.ds(*table[side]) for side in (a, b))

    first_halo = []
    for k, (a, b) in enumerate(sides):
        first_halo.append(
            pltpu.make_async_remote_copy(
                src_ref=fixed.at[spans({-1: (1, 1), 0: (1, 2), 1: (2, 1)}, a, b)],
                dst_ref=fixed.at[spans({-1: (3, 1), 0: (1, 2), 1: (0, 1)}, a, b)],
                send_sem=halo_send.at[0, k],
                recv_sem=halo_recv.at[0, k],
                device_id=(wrap(mx + a), wrap(my + b)),
                device_id_type=MESH,
            )
        )
    for copy in first_halo:
        copy.start()
    lax.fori_loop(1, SIDE, second, 0)

    taken = {-1: (2, 1), 0: (0, 3), 1: (0, 2)}
    inner = {-1: (0, 1), 0: (0, 3), 1: (0, 2)}

    def part_copies():
        copies = []
        for a, b in sides:
            k = sides.index((-a, -b))
            copies.append(
                pltpu.make_async_remote_copy(
                    src_ref=part.at[spans(taken, -a, -b)],
                    dst_ref=inbox.at[(k, *spans(inner, -a, -b))],
                    send_sem=halo_send.at[1, k],
                    recv_sem=halo_recv.at[1, k],
                    device_id=(wrap(mx + a), wrap(my + b)),
                    device_id_type=MESH,
                )
            )
        return copies

    pick = [((lane // 8 + dz + 16) % 16) * 8 + row for dz in (-1, 0, 1)]

    def expanded(line, k):
        return jnp.take_along_axis(
            jnp.broadcast_to(line, (8, 128)), pick[k], axis=1, mode="promise_in_bounds"
        )

    def grow_static(col, carry):
        tile = fixed[col // 4, lax.rem(col, 4)]
        lines = [tile[c : c + 1] + 1.0 + tile[c + 3 : c + 4] for c in range(3)] + [tile[6:7]]
        for k in range(3):
            for c in range(4):
                value = expanded(lines[c], k)
                if c == 2:
                    value = value + 16.0 * (k - 1)
                near_static[col, k, c] = value
        return carry

    def grow_moving(it):
        def body(col, carry):
            tile = moving[it, col // 4, lax.rem(col, 4)]
            for k in range(3):
                for c in range(3):
                    near_moving[col, k, c] = expanded(tile[c : c + 1], k)
            return carry

        lax.fori_loop(0, 16, body, 0)

    tall = lax.broadcasted_iota(jnp.int32, (N, 128), 0)
    low = lax.broadcasted_iota(jnp.int32, (SIDE, 128), 0)
    cell_z = lax.broadcasted_iota(jnp.int32, (1, 128), 1) // 8 * 16

    def weights(col):
        ex = col // 3
        ey = lax.rem(col, 3)
        tile = fixed[ex, ey]
        anchor = tile[0:3].astype(jnp.int32)
        value, slope = zip(*[spline(tile[c + 3 : c + 4]) for c in range(3)])
        place_x = low - (anchor[0:1] + (ex - 1) * 8)
        place_y = low - (anchor[1:2] + (ey - 1) * 8)
        place_z = (tall - (anchor[2:3] + cell_z)) & (N - 1)
        wx, sx = placed(place_x, value[0]), placed(place_x, slope[0])
        wy, sy = placed(place_y, value[1]), placed(place_y, slope[1])
        for x in range(SIDE):
            rows = pl.ds(x * SIDE, SIDE)
            prod[col, 0, rows] = sx[x : x + 1] * wy
            prod[col, 1, rows] = wx[x : x + 1] * sy
            prod[col, 2, rows] = wx[x : x + 1] * wy
        for k, source in enumerate((value[2], slope[2])):
            full = placed(place_z, source)
            lanes = pl.ds(pl.multiple_of(col * N + 128 * k, 128), 128)
            wz_hi[:, lanes], wz_lo[:, lanes] = halves(full)
            wt_hi[lanes, :], wt_lo[lanes, :] = halves(full.T)

    def weights_own(i, carry):
        weights((1 + i // 2) * 3 + 1 + lax.rem(i, 2))
        return carry

    def weights_other(i, carry):
        weights(i + 2 * (i // 4))
        return carry

    lax.fori_loop(0, 4, weights_own, 0)
    for copy in first_halo:
        copy.wait()
    lax.fori_loop(0, 5, weights_other, 0)

    def first_moment(col, carry):
        tile = fixed[col // 4, lax.rem(col, 4)]
        moving[0, col // 4, lax.rem(col, 4)] = tile[7:8] * tile[8:16]
        return carry

    lax.fori_loop(0, 16, first_moment, 0)

    def pairs(item, carry):
        q = item // 9
        nb = lax.rem(item, 9)
        cx = q // 2
        cy = lax.rem(q, 2)
        dx = nb // 3 - 1
        dy = lax.rem(nb, 3) - 1
        tile = fixed[cx + 1, cy + 1]
        here = [tile[c : c + 1] + 1.0 + tile[c + 3 : c + 4] for c in range(3)]
        here[0] = here[0] - (8 * dx).astype(F32)
        here[1] = here[1] - (8 * dy).astype(F32)
        mine = tile[6:7]
        col = (cx + 1 + dx) * 4 + cy + 1 + dy
        for k in range(3):
            apart = [here[c] - near_static[col, k, c] for c in range(3)]
            square = apart[0] * apart[0] + apart[1] * apart[1] + apart[2] * apart[2]
            root = lax.rsqrt(mine * near_static[col, k, 3])
            if k == 1:
                same = (row == lane % 8) & (nb == 4)
                square = jnp.where(same, 1.0, square)
            c1, c2 = pair_coefficients(square, root)
            if k == 1:
                c1 = jnp.where(same, 0.0, c1)
                c2 = jnp.where(same, 0.0, c2)
            scaled = [c2 * apart[c] for c in range(3)]
            tensor[item, k, 0] = scaled[0] * apart[0] - c1
            tensor[item, k, 1] = scaled[1] * apart[1] - c1
            tensor[item, k, 2] = scaled[2] * apart[2] - c1
            tensor[item, k, 3] = scaled[0] * apart[1]
            tensor[item, k, 4] = scaled[0] * apart[2]
            tensor[item, k, 5] = scaled[1] * apart[2]
        return carry

    def near_field(it):
        grow_moving(it)

        def body(q, carry):
            cx = q // 2
            cy = lax.rem(q, 2)

            def inner(nb, total):
                fx, fy, fz = total
                col = (cx + nb // 3) * 4 + cy + lax.rem(nb, 3)
                item = q * 9 + nb
                for k in range(3):
                    vx, vy, vz = [near_moving[col, k, c] for c in range(3)]
                    xx, yy, zz, xy, xz, yz = [tensor[item, k, c] for c in range(6)]
                    fx = fx + (xx * vx + xy * vy + xz * vz)
                    fy = fy + (xy * vx + yy * vy + yz * vz)
                    fz = fz + (xz * vx + yz * vy + zz * vz)
                return fx, fy, fz

            zero = jnp.zeros((8, 128), F32)
            sums = lax.fori_loop(0, 9, inner, (zero, zero, zero))
            near[q] = jnp.concatenate(
                [jnp.sum(s, axis=0, keepdims=True) for s in sums]
                + [jnp.zeros((5, 128), F32)],
                axis=0,
            )
            return carry

        lax.fori_loop(0, 4, body, 0)

    def exchange(source, target, k):
        def copy(t):
            return pltpu.make_async_remote_copy(
                src_ref=source.at[t],
                dst_ref=target.at[me],
                send_sem=send_s.at[k],
                recv_sem=recv_s.at[k],
                device_id=(t // SIDE, lax.rem(t, SIDE)),
                device_id_type=MESH,
            )

        def send(i, carry):
            copy(lax.rem(me + i, N)).start()
            return carry

        lax.fori_loop(1, N, send, 0)
        target[me] = source[me]

    def arrive(source, target, k):
        pltpu.make_async_remote_copy(
            src_ref=source.at[pl.ds(0, N - 1)],
            dst_ref=target.at[pl.ds(0, N - 1)],
            send_sem=send_s.at[k],
            recv_sem=recv_s.at[k],
            device_id=(mx, wrap(my + 1)),
            device_id_type=MESH,
        ).wait()

    def wave(k):
        return waves[0, N * k : N * (k + 1)], waves[1, N * k : N * (k + 1)]

    def put_rows(ref, value):
        ref[:, 0, :] = value[:, :128]
        ref[:, 1, :] = value[:, 128:]

    def get_rows(ref):
        return jnp.concatenate([ref[:, 0, :], ref[:, 1, :]], axis=1)

    def filtered(value):
        cosine = wave(1)
        sine = wave(2)
        upper = tuple(
            jnp.concatenate([c[:HALF], s[:HALF]], axis=0) for c, s in zip(cosine, sine)
        )
        both = product(upper, halves(value))
        re, im = both[:HALF], both[HALF:]
        tr, ti = plane[0], plane[1]
        both = halves(jnp.concatenate([re * tr - im * ti, re * ti + im * tr], axis=0))
        by_cosine = product(both, cosine)
        by_sine = product(both, sine)
        re = by_cosine[:HALF] - by_sine[HALF:]
        im = by_sine[:HALF] + by_cosine[HALF:]
        line = jnp.zeros((1, 128), F32) + me.astype(F32)
        signed = jnp.where(line < N // 2, line, line - N) * (1.0 / N)
        height = signed * signed
        bend = 2.0 + jnp.cos(line * (2.0 * math.pi / N))
        strength = jnp.exp(-((math.pi / BETA) ** 2) * height) * 9.0 / (bend * bend)
        height = jnp.concatenate([height, height], axis=1)
        strength = jnp.concatenate([strength, strength], axis=1)
        square = plane[3] + height
        centre = square == 0.0
        green = jnp.where(
            centre, 0.0, plane[2] * strength / jnp.where(centre, 1.0, square)
        )
        both = halves(jnp.concatenate([re * green, im * green], axis=0))
        by_cosine = product(both, cosine)
        by_sine = product(both, sine)
        re = by_cosine[:HALF] + by_sine[HALF:]
        im = by_cosine[HALF:] - by_sine[:HALF]
        first = halves(re * tr + im * ti)
        other = halves(im * tr - re * ti)
        cosine = tuple(c[:, :HALF] for c in cosine)
        sine = tuple(c[:, :HALF] for c in sine)
        return product(cosine, first) + product(sine, other)

    def iteration(it, carry):
        for group in range(3):
            for col in range(3 * group, 3 * group + 3):
                tile = moving[it, col // 3, col % 3]
                plain = tile[0:1] * prod[col, 0] + tile[1:2] * prod[col, 1]
                steep = tile[2:3] * prod[col, 2]
                left = slice(col * N, col * N + 128)
                right = slice(col * N + 128, col * N + N)
                p_hi[:, left], p_lo[:, left] = halves(plain)
                p_hi[:, right], p_lo[:, right] = halves(steep)
            span = slice(3 * N * group, 3 * N * (group + 1))
            term = product((p_hi[:, span], p_lo[:, span]), (wt_hi[span], wt_lo[span]))
            if group == 0:
                spread[...] = term
            else:
                spread[...] += term

        @pl.when(it == 0)
        def _():
            for copy in table_copies:
                copy.wait()

        put_rows(send_a, product(wave(0), halves(spread[...]), NT))

        @pl.when(it == 0)
        def _():
            pl.semaphore_wait(second_level, SIDE - 1)

        exchange(send_a, land_a.at[it], 2 * it)

        @pl.when(it == 0)
        def _():
            lax.fori_loop(0, 16, grow_static, 0)
            lax.fori_loop(0, 36, pairs, 0)

        arrive(send_a, land_a.at[it], 2 * it)
        put_rows(send_b, filtered(get_rows(land_a.at[it])))
        exchange(send_b, land_b.at[it], 2 * it + 1)
        near_field(it)
        arrive(send_b, land_b.at[it], 2 * it + 1)
        potential = product(wave(0), halves(get_rows(land_b.at[it])))
        turned = halves(potential.T)

        def gather(col):
            lanes = slice(col * N, col * N + N)
            sampled = product(turned, (wz_hi[:, lanes], wz_lo[:, lanes]))
            plain = sampled[:, :128]
            steep = sampled[:, 128:]
            ex, ey = col // 3, col % 3
            total = jnp.concatenate(
                [
                    -jnp.sum(prod[col, 0] * plain, axis=0, keepdims=True),
                    -jnp.sum(prod[col, 1] * plain, axis=0, keepdims=True),
                    -jnp.sum(prod[col, 2] * steep, axis=0, keepdims=True),
                    jnp.zeros((5, 128), F32),
                ],
                axis=0,
            )
            if ex >= 1 and ey >= 1:
                total = total + near[2 * ex + ey - 3] + SELF_GAIN * moving[it, ex, ey]
            part[ex, ey] = total

        for col in (0, 1, 2, 3, 6):
            gather(col)

        def last_copies():
            copies = []
            for k, (a, b) in enumerate(((1, 0), (0, 1), (1, 1))):
                span = {0: (1, 2), 1: (0, 1)}
                land = {0: (0, 2), 1: (0, 1)}
                copies.append(
                    pltpu.make_async_remote_copy(
                        src_ref=part.at[spans(span, a, b)],
                        dst_ref=last_in.at[(k, *spans(land, a, b))],
                        send_sem=part_send.at[k],
                        recv_sem=part_recv.at[k],
                        device_id=(wrap(mx - a), wrap(my - b)),
                        device_id_type=MESH,
                    )
                )
            return copies

        @pl.when(it == ITERS - 1)
        def _():
            for copy in last_copies():
                copy.start()

        for col in (4, 5, 7, 8):
            gather(col)

        @pl.when(it == 0)
        def _():
            copies = part_copies()
            for copy in copies:
                copy.start()
            for copy in copies:
                copy.wait()
            reach = {0: ((-1, 0), (0, 0)), 1: ((0, 1),), 2: ((0, 2), (1, 0)), 3: ((1, 1),)}
            for ex in range(4):
                for ey in range(4):
                    total = jnp.zeros((8, 128), F32)
                    for a, i in reach[ex]:
                        for b, j in reach[ey]:
                            if a == 0 and b == 0:
                                total = total + part[i, j]
                            else:
                                total = total + inbox[sides.index((a, b)), i, j]
                    moving[1, ex, ey] = fixed[ex, ey, 7:8] * (fixed[ex, ey, 8:16] + total)

        @pl.when(it == ITERS - 1)
        def _():
            for copy in last_copies():
                copy.wait()
            for cx in range(2):
                for cy in range(2):
                    total = part[cx + 1, cy + 1]
                    if cx == 1:
                        total = total + last_in[0, 0, cy]
                    if cy == 1:
                        total = total + last_in[1, cx, 0]
                    if cx == 1 and cy == 1:
                        total = total + last_in[2, 0, 0]
                    tile = fixed[cx + 1, cy + 1]
                    result = tile[7:8] * (tile[8:16] + total)
                    for c in range(3):
                        out[c, cx, cy : cy + 1] = result[c : c + 1]

        return carry

    lax.fori_loop(0, ITERS, iteration, 0)


def shards(cotangent, polarizability, site_offset, site_fraction, cell_count):
    vmem = pl.BlockSpec(memory_space=pltpu.VMEM)

    def room(*shape, dtype=F32):
        return pltpu.VMEM(shape, dtype)

    dma = pltpu.SemaphoreType.DMA
    return pl.pallas_call(
        kernel,
        out_shape=jax.ShapeDtypeStruct((3, 2, 2, 128), F32),
        in_specs=[vmem] * 5 + [pl.BlockSpec(memory_space=pl.ANY)] * 2,
        out_specs=vmem,
        scratch_shapes=[
            room(2, 3 * N, N, dtype=BF16),
            room(4, HALF, N),
            room(4, 4, 16, 128),
            room(2, 4, 4, 8, 128),
            room(9, 3, N, 128),
            room(N, 9 * N, dtype=BF16),
            room(N, 9 * N, dtype=BF16),
            room(9 * N, N, dtype=BF16),
            room(9 * N, N, dtype=BF16),
            room(N, 9 * N, dtype=BF16),
            room(N, 9 * N, dtype=BF16),
            room(N, N),
            room(N, 2, 128),
            room(N, 2, 128),
            room(2, N, 2, 128),
            room(2, N, 2, 128),
            room(16, 3, 4, 8, 128),
            room(16, 3, 3, 8, 128),
            room(36, 3, 6, 8, 128),
            room(4, 8, 128),
            room(3, 3, 8, 128),
            room(8, 3, 3, 8, 128),
            room(3, 2, 2, 8, 128),
            dma((2,)),
            dma((4,)),
            dma((4,)),
            dma((2, 8)),
            dma((2, 8)),
            dma((3,)),
            dma((3,)),
            pltpu.SemaphoreType.REGULAR,
        ],
        compiler_params=pltpu.CompilerParams(
            collective_id=0, has_side_effects=True, vmem_limit_bytes=56 * 1024 * 1024
        ),
    )(
        cotangent,
        polarizability,
        site_offset,
        site_fraction,
        cell_count,
        *[jnp.asarray(table) for table in TABLES],
    )


def solution(mesh):
    return jax.shard_map(
        shards,
        mesh=mesh,
        in_specs=(
            P(None, "gx", "gy", None),
            P("gx", "gy", None),
            P(None, "gx", "gy", None),
            P(None, "gx", "gy", None),
            P("gx", "gy", None),
        ),
        out_specs=P(None, "gx", "gy", None),
        check_vma=False,
    )
```

```python
import math

import jax
import jax.numpy as jnp
import ml_dtypes
import numpy as np
from jax import lax
from jax.experimental import pallas as pl
from jax.experimental.pallas import tpu as pltpu
from jax.sharding import PartitionSpec as P

BETA = 0.7
THOLE = 0.39
ROOT_PI = 1.7724538509055159
SELF_GAIN = 4.0 * BETA * BETA * BETA / (3.0 * ROOT_PI)
ITERS = 2
N = 256
SIDE = 16
HALF = SIDE * (SIDE // 2 + 1)
MESH = pl.DeviceIdType.MESH
F32 = jnp.float32
BF16 = jnp.bfloat16

ERFC_P = (
    2.326819970068386e-2,
    -1.387039388740657e-1,
    3.687424674597105e-1,
    -5.824733027278666e-1,
    6.210004621745983e-1,
    -4.944515323274145e-1,
    3.404879937665872e-1,
    -2.741127028184656e-1,
    5.638259427386472e-1,
)
ERFC_R = (
    -1.047766399936249e1,
    1.297719955372516e1,
    -7.495518717768503e0,
    2.921019019210786e0,
    -1.015265279202700e0,
    4.218463358204948e-1,
    -2.820767439740514e-1,
    5.641895067754075e-1,
)
ERF_T = (
    7.853861353153693e-5,
    -8.010193625184903e-4,
    5.188327685732524e-3,
    -2.685381193529856e-2,
    1.128358514861418e-1,
    -3.761262582423300e-1,
    1.128379165726710e0,
)


def halves_np(table):
    high = table.astype(np.float32).astype(ml_dtypes.bfloat16)
    low = (table - high.astype(np.float64)).astype(np.float32).astype(ml_dtypes.bfloat16)
    return high, low


def tables():
    grid = np.arange(N)
    angle = 2.0 * math.pi / N * (grid[:, None] * grid[None, :] % N)
    hartley = np.cos(angle) + np.sin(angle)
    short = np.arange(SIDE)
    pair = (
        short[:, None, None, None] * short[None, None, :, None]
        + short[None, :, None, None] * short[None, None, None, :]
    ).reshape(N, N)
    outer = 2.0 * math.pi / SIDE * (pair % SIDE)
    twist = 2.0 * math.pi / N * (pair % N)

    def part(freq):
        signed = np.where(2 * freq < N, freq, freq - N) / N
        factor = 9.0 / (2.0 + np.cos(2.0 * math.pi * freq / N)) ** 2
        return signed * signed, factor

    low_x = short[:, None, None, None]
    low_y = short[None, :, None, None]
    freq_x = (low_x + SIDE * short[None, None, :, None]) + 0 * low_y
    freq_y = (low_y + SIDE * short[None, None, None, :]) + 0 * low_x
    square_x, factor_x = part(freq_x)
    square_y, factor_y = part(freq_y)
    square = (square_x + square_y).reshape(N, N)
    gain = (
        np.exp(-((math.pi / BETA) ** 2) * (square_x + square_y)) * factor_x * factor_y / math.pi
    ).reshape(N, N) / float(N * N * N)
    twice = np.where((grid // SIDE == 0) | (grid // SIDE == SIDE // 2), 1.0, 2.0)
    gain = gain * twice[:, None]
    waves = np.stack(halves_np(np.concatenate([hartley, np.cos(outer), -np.sin(outer)], axis=0)))
    plane = np.stack([np.cos(twist), -np.sin(twist), gain, square])[:, :HALF].astype(np.float32)
    return waves, plane


TABLES = tables()

SUPPORT = {0: (0, 3), 1: (0, 11), 2: (8, 16)}


def ring(offset, count):
    return min(offset, count - offset)


ROUTES = [
    (dy, dx, dz, dc)
    for dz in range(8)
    for dy in range(4)
    for dx in range(4)
    for dc in range(2)
    if (dy, dx, dz, dc) != (0, 0, 0, 0)
]
ROUTES.sort(key=lambda r: -(ring(r[0], 4) + ring(r[1], 4) + ring(r[2], 8)))

NN = (((1,), (0,)), ((), ()))
NT = (((1,), (1,)), ((), ()))


def halves(value):
    high = value.astype(BF16)
    return high, (value - high.astype(F32)).astype(BF16)


def product(left, right, dims=NN):
    def dot(a, b):
        return lax.dot_general(a, b, dims, preferred_element_type=F32)

    count = left[0].shape[0]
    both = dot(jnp.concatenate(left, axis=0), right[0])
    return both[:count] + (both[count:] + dot(left[0], right[1]))


def polynomial(terms, value):
    total = jnp.full_like(value, terms[0])
    for term in terms[1:]:
        total = total * value + term
    return total


def pair_coefficients(square, root):
    inverse = lax.rsqrt(square)
    distance = square * inverse
    inverse_square = 1.0 / square
    argument = BETA * distance
    steep = argument * argument
    bell = jnp.exp(-steep)
    ratio = inverse * (1.0 / BETA)
    small = ratio * ratio
    tail = jnp.where(
        argument < 2.0, polynomial(ERFC_P, small), polynomial(ERFC_R, small)
    )
    erfc = jnp.where(
        argument < 1.0,
        1.0 - argument * polynomial(ERF_T, steep),
        bell * ratio * tail,
    )
    gauss = (2.0 * BETA / ROOT_PI) * bell
    first = (erfc * inverse + gauss) * inverse_square
    second = (3.0 * first + (2.0 * BETA * BETA) * gauss) * inverse_square
    scaled = THOLE * square * distance * root
    damping = jnp.exp(-scaled)
    inverse_cube = inverse_square * inverse
    first = first - damping * inverse_cube
    second = second - 3.0 * (1.0 + scaled) * damping * inverse_cube * inverse_square
    return first, second


def spline(f):
    rest = 1.0 - f
    square = f * f
    cube = square * f
    values = (
        rest * rest * rest / 6.0,
        (3.0 * cube - 6.0 * square + 4.0) / 6.0,
        (-3.0 * cube + 3.0 * square + 3.0 * f + 1.0) / 6.0,
        cube / 6.0,
    )
    slopes = (
        -0.5 * rest * rest,
        0.5 * (3.0 * square - 4.0 * f),
        0.5 * (-3.0 * square + 2.0 * f + 1.0),
        0.5 * square,
    )
    return values, slopes


def placed(place, weights):
    total = jnp.where(place == 0, weights[0], 0.0)
    for order in range(1, 4):
        total = jnp.where(place == order, weights[order], total)
    return total


def kernel(
    cot_far, pol_far, off_far, frac_far, cnt_far, waves_far, plane_far,
    out,
    cot, pol, off, frac, cnt, waves, plane, fixed, moving, prod, wz_hi, wz_lo, wt_hi, wt_lo, p_hi, p_lo, spread,
    send_a, send_b, land_a, land_b, near_static, near_moving, tensor, near, part, inbox, last_in,
    table_sem, send_s, recv_s, halo_send, halo_recv, part_send, part_recv, second_level,
):
    mx = lax.axis_index("gx")
    my = lax.axis_index("gy")
    me = mx * SIDE + my

    def wrap(i):
        return lax.rem(i + SIDE, SIDE)

    arguments = [
        pltpu.make_async_copy(source, target, table_sem.at[2 + k])
        for k, (source, target) in enumerate(
            ((cot_far, cot), (pol_far, pol), (off_far, off), (frac_far, frac), (cnt_far, cnt))
        )
    ]
    table_copies = [
        pltpu.make_async_copy(waves_far, waves, table_sem.at[0]),
        pltpu.make_async_copy(plane_far, plane, table_sem.at[1]),
    ]
    for copy in arguments + table_copies:
        copy.start()

    entry = pltpu.get_barrier_semaphore()

    def greet(i, carry):
        pl.semaphore_signal(entry, inc=1, device_id=(wrap(mx + i), my), device_id_type=MESH)
        pl.semaphore_signal(entry, inc=1, device_id=(mx, wrap(my + i)), device_id_type=MESH)
        return carry

    lax.fori_loop(1, SIDE, greet, 0)
    for a in (-1, 1):
        for b in (-1, 1):
            pl.semaphore_signal(
                entry, inc=1, device_id=(wrap(mx + a), wrap(my + b)), device_id_type=MESH
            )

    for copy in arguments:
        copy.wait()
    lane = lax.broadcasted_iota(jnp.int32, (8, 128), 1)
    row = lax.broadcasted_iota(jnp.int32, (8, 128), 0)
    expand = (
        lax.broadcasted_iota(jnp.int32, (16, 128), 1) // 8
        == lax.broadcasted_iota(jnp.int32, (16, 128), 0)
    ).astype(F32)
    slot = (lax.broadcasted_iota(jnp.int32, (2, 128), 1) % 8).astype(F32)
    for cx in range(2):
        counts = jnp.dot(cnt[cx].astype(F32), expand, preferred_element_type=F32)
        weight = jnp.where(slot < counts, 1.0, 0.0) * pol[cx]
        for cy in range(2):
            here = slice(cy, cy + 1)
            fixed[cx + 1, cy + 1] = jnp.concatenate(
                [off[c, cx, here].astype(F32) for c in range(3)]
                + [frac[c, cx, here] for c in range(3)]
                + [pol[cx, here], weight[here]]
                + [cot[c, cx, here] for c in range(3)]
                + [jnp.zeros((5, 128), F32)],
                axis=0,
            )

    pl.semaphore_wait(entry, 2 * (SIDE - 1) + 4)

    def second(i, carry):
        pl.semaphore_signal(
            second_level, inc=1, device_id=(wrap(mx + i), my), device_id_type=MESH
        )
        return carry

    sides = [(a, b) for a in (-1, 0, 1) for b in (-1, 0, 1) if (a, b) != (0, 0)]

    def spans(table, a, b):
        return tuple(pl.ds(*table[side]) for side in (a, b))

    first_halo = []
    for k, (a, b) in enumerate(sides):
        first_halo.append(
            pltpu.make_async_remote_copy(
                src_ref=fixed.at[spans({-1: (1, 1), 0: (1, 2), 1: (2, 1)}, a, b)],
                dst_ref=fixed.at[spans({-1: (3, 1), 0: (1, 2), 1: (0, 1)}, a, b)],
                send_sem=halo_send.at[0, k],
                recv_sem=halo_recv.at[0, k],
                device_id=(wrap(mx + a), wrap(my + b)),
                device_id_type=MESH,
            )
        )
    for copy in first_halo:
        copy.start()
    lax.fori_loop(1, SIDE, second, 0)

    taken = {-1: (2, 1), 0: (0, 3), 1: (0, 2)}
    inner = {-1: (0, 1), 0: (0, 3), 1: (0, 2)}

    def part_copies():
        copies = []
        for a, b in sides:
            k = sides.index((-a, -b))
            copies.append(
                pltpu.make_async_remote_copy(
                    src_ref=part.at[spans(taken, -a, -b)],
                    dst_ref=inbox.at[(k, *spans(inner, -a, -b))],
                    send_sem=halo_send.at[1, k],
                    recv_sem=halo_recv.at[1, k],
                    device_id=(wrap(mx + a), wrap(my + b)),
                    device_id_type=MESH,
                )
            )
        return copies

    pick = [((lane // 8 + dz + 16) % 16) * 8 + row for dz in (-1, 0, 1)]

    def expanded(line, k):
        return jnp.take_along_axis(
            jnp.broadcast_to(line, (8, 128)), pick[k], axis=1, mode="promise_in_bounds"
        )

    def grow_static(col, carry):
        tile = fixed[col // 4, lax.rem(col, 4)]
        lines = [tile[c : c + 1] + 1.0 + tile[c + 3 : c + 4] for c in range(3)] + [tile[6:7]]
        for k in range(3):
            for c in range(4):
                value = expanded(lines[c], k)
                if c == 2:
                    value = value + 16.0 * (k - 1)
                near_static[col, k, c] = value
        return carry

    def grow_moving(it):
        def body(col, carry):
            tile = moving[it, col // 4, lax.rem(col, 4)]
            for k in range(3):
                for c in range(3):
                    near_moving[col, k, c] = expanded(tile[c : c + 1], k)
            return carry

        lax.fori_loop(0, 16, body, 0)

    tall = lax.broadcasted_iota(jnp.int32, (N, 128), 0)
    low = lax.broadcasted_iota(jnp.int32, (SIDE, 128), 0)
    cell_z = lax.broadcasted_iota(jnp.int32, (1, 128), 1) // 8 * 16

    def weights(ex, ey):
        col = ex * 3 + ey
        tile = fixed[ex, ey]
        anchor = tile[0:3].astype(jnp.int32)
        value, slope = zip(*[spline(tile[c + 3 : c + 4]) for c in range(3)])
        place_x = low - (anchor[0:1] + (ex - 1) * 8)
        place_y = low - (anchor[1:2] + (ey - 1) * 8)
        place_z = (tall - (anchor[2:3] + cell_z)) & (N - 1)
        wx, sx = placed(place_x, value[0]), placed(place_x, slope[0])
        wy, sy = placed(place_y, value[1]), placed(place_y, slope[1])
        for x in range(*SUPPORT[ex]):
            rows = pl.ds(x * SIDE, SIDE)
            prod[col, 0, rows] = sx[x : x + 1] * wy
            prod[col, 1, rows] = wx[x : x + 1] * sy
            prod[col, 2, rows] = wx[x : x + 1] * wy
        for k, source in enumerate((value[2], slope[2])):
            full = placed(place_z, source)
            lanes = pl.ds(pl.multiple_of(col * N + 128 * k, 128), 128)
            wz_hi[:, lanes], wz_lo[:, lanes] = halves(full)
            wt_hi[lanes, :], wt_lo[lanes, :] = halves(full.T)

    def weights_of(ex):
        def body(ey, carry):
            weights(ex, ey)
            return carry

        return body

    lax.fori_loop(1, 3, weights_of(1), 0)
    lax.fori_loop(1, 3, weights_of(2), 0)
    for copy in first_halo:
        copy.wait()
    lax.fori_loop(0, 3, weights_of(0), 0)
    weights(1, 0)
    weights(2, 0)

    def first_moment(col, carry):
        tile = fixed[col // 4, lax.rem(col, 4)]
        moving[0, col // 4, lax.rem(col, 4)] = tile[7:8] * tile[8:16]
        return carry

    lax.fori_loop(0, 16, first_moment, 0)

    def pairs(item, carry):
        q = item // 9
        nb = lax.rem(item, 9)
        cx = q // 2
        cy = lax.rem(q, 2)
        dx = nb // 3 - 1
        dy = lax.rem(nb, 3) - 1
        tile = fixed[cx + 1, cy + 1]
        here = [tile[c : c + 1] + 1.0 + tile[c + 3 : c + 4] for c in range(3)]
        here[0] = here[0] - (8 * dx).astype(F32)
        here[1] = here[1] - (8 * dy).astype(F32)
        mine = tile[6:7]
        col = (cx + 1 + dx) * 4 + cy + 1 + dy
        for k in range(3):
            apart = [here[c] - near_static[col, k, c] for c in range(3)]
            square = apart[0] * apart[0] + apart[1] * apart[1] + apart[2] * apart[2]
            root = lax.rsqrt(mine * near_static[col, k, 3])
            if k == 1:
                same = (row == lane % 8) & (nb == 4)
                square = jnp.where(same, 1.0, square)
            c1, c2 = pair_coefficients(square, root)
            if k == 1:
                c1 = jnp.where(same, 0.0, c1)
                c2 = jnp.where(same, 0.0, c2)
            scaled = [c2 * apart[c] for c in range(3)]
            tensor[item, k, 0] = scaled[0] * apart[0] - c1
            tensor[item, k, 1] = scaled[1] * apart[1] - c1
            tensor[item, k, 2] = scaled[2] * apart[2] - c1
            tensor[item, k, 3] = scaled[0] * apart[1]
            tensor[item, k, 4] = scaled[0] * apart[2]
            tensor[item, k, 5] = scaled[1] * apart[2]
        return carry

    def near_field(it):
        grow_moving(it)

        def body(q, carry):
            cx = q // 2
            cy = lax.rem(q, 2)

            def inner(nb, total):
                fx, fy, fz = total
                col = (cx + nb // 3) * 4 + cy + lax.rem(nb, 3)
                item = q * 9 + nb
                for k in range(3):
                    vx, vy, vz = [near_moving[col, k, c] for c in range(3)]
                    xx, yy, zz, xy, xz, yz = [tensor[item, k, c] for c in range(6)]
                    fx = fx + (xx * vx + xy * vy + xz * vz)
                    fy = fy + (xy * vx + yy * vy + yz * vz)
                    fz = fz + (xz * vx + yz * vy + zz * vz)
                return fx, fy, fz

            zero = jnp.zeros((8, 128), F32)
            sums = lax.fori_loop(0, 9, inner, (zero, zero, zero))
            near[q] = jnp.concatenate(
                [jnp.sum(s, axis=0, keepdims=True) for s in sums]
                + [jnp.zeros((5, 128), F32)],
                axis=0,
            )
            return carry

        lax.fori_loop(0, 4, body, 0)

    def exchange(source, target, k):
        for dy, dx, dz, dc in ROUTES:
            to_y = lax.rem(mx // 4 + dy, 4)
            to_x = lax.rem(my // 8 * 2 + lax.rem(mx // 2, 2) + dx, 4)
            to_z = lax.rem(my + dz, 8)
            to_core = lax.rem(mx + dc, 2)
            gx = to_y * 4 + lax.rem(to_x, 2) * 2 + to_core
            gy = to_x // 2 * 8 + to_z
            pltpu.make_async_remote_copy(
                src_ref=source.at[gx * SIDE + gy],
                dst_ref=target.at[me],
                send_sem=send_s.at[k],
                recv_sem=recv_s.at[k],
                device_id=(gx, gy),
                device_id_type=MESH,
            ).start()

        target[me] = source[me]

    def arrive(source, target, k):
        pltpu.make_async_remote_copy(
            src_ref=source.at[pl.ds(0, N - 1)],
            dst_ref=target.at[pl.ds(0, N - 1)],
            send_sem=send_s.at[k],
            recv_sem=recv_s.at[k],
            device_id=(mx, wrap(my + 1)),
            device_id_type=MESH,
        ).wait()

    def wave(k):
        return waves[0, N * k : N * (k + 1)], waves[1, N * k : N * (k + 1)]

    def put_rows(ref, value):
        ref[:, 0, :] = value[:, :128]
        ref[:, 1, :] = value[:, 128:]

    def get_rows(ref):
        return jnp.concatenate([ref[:, 0, :], ref[:, 1, :]], axis=1)

    def filtered(value):
        cosine = wave(1)
        sine = wave(2)
        upper = tuple(
            jnp.concatenate([c[:HALF], s[:HALF]], axis=0) for c, s in zip(cosine, sine)
        )
        both = product(upper, halves(value))
        re, im = both[:HALF], both[HALF:]
        tr, ti = plane[0], plane[1]
        both = halves(jnp.concatenate([re * tr - im * ti, re * ti + im * tr], axis=0))
        by_cosine = product(both, cosine)
        by_sine = product(both, sine)
        re = by_cosine[:HALF] - by_sine[HALF:]
        im = by_sine[:HALF] + by_cosine[HALF:]
        line = jnp.zeros((1, 128), F32) + me.astype(F32)
        signed = jnp.where(line < N // 2, line, line - N) * (1.0 / N)
        height = signed * signed
        bend = 2.0 + jnp.cos(line * (2.0 * math.pi / N))
        strength = jnp.exp(-((math.pi / BETA) ** 2) * height) * 9.0 / (bend * bend)
        height = jnp.concatenate([height, height], axis=1)
        strength = jnp.concatenate([strength, strength], axis=1)
        square = plane[3] + height
        centre = square == 0.0
        green = jnp.where(
            centre, 0.0, plane[2] * strength / jnp.where(centre, 1.0, square)
        )
        both = halves(jnp.concatenate([re * green, im * green], axis=0))
        by_cosine = product(both, cosine)
        by_sine = product(both, sine)
        re = by_cosine[:HALF] + by_sine[HALF:]
        im = by_cosine[HALF:] - by_sine[:HALF]
        first = halves(re * tr + im * ti)
        other = halves(im * tr - re * ti)
        cosine = tuple(c[:, :HALF] for c in cosine)
        sine = tuple(c[:, :HALF] for c in sine)
        return product(cosine, first) + product(sine, other)

    def iteration(it, carry):
        for ex in (1, 2, 0):
            rows = slice(SUPPORT[ex][0] * SIDE, SUPPORT[ex][1] * SIDE)
            for ey in range(3):
                col = 3 * ex + ey
                tile = moving[it, ex, ey]
                plain = tile[0:1] * prod[col, 0, rows] + tile[1:2] * prod[col, 1, rows]
                steep = tile[2:3] * prod[col, 2, rows]
                left = slice(col * N, col * N + 128)
                right = slice(col * N + 128, col * N + N)
                p_hi[rows, left], p_lo[rows, left] = halves(plain)
                p_hi[rows, right], p_lo[rows, right] = halves(steep)
            span = slice(3 * N * ex, 3 * N * (ex + 1))
            term = product((p_hi[rows, span], p_lo[rows, span]), (wt_hi[span], wt_lo[span]))
            if ex == 1:
                spread[rows] = term
                spread[rows.stop :] = jnp.zeros((N - rows.stop, N), F32)
            else:
                spread[rows] += term

        @pl.when(it == 0)
        def _():
            for copy in table_copies:
                copy.wait()

        put_rows(send_a, product(wave(0), halves(spread[...]), NT))

        @pl.when(it == 0)
        def _():
            pl.semaphore_wait(second_level, SIDE - 1)

        exchange(send_a, land_a.at[it], 2 * it)

        @pl.when(it == 0)
        def _():
            lax.fori_loop(0, 16, grow_static, 0)
            lax.fori_loop(0, 36, pairs, 0)

        arrive(send_a, land_a.at[it], 2 * it)
        put_rows(send_b, filtered(get_rows(land_a.at[it])))
        exchange(send_b, land_b.at[it], 2 * it + 1)
        near_field(it)
        arrive(send_b, land_b.at[it], 2 * it + 1)
        potential = product(wave(0), halves(get_rows(land_b.at[it])))
        turned = halves(potential.T)

        def gather(col):
            lanes = slice(col * N, col * N + N)
            ex, ey = col // 3, col % 3
            rows = slice(SUPPORT[ex][0] * SIDE, SUPPORT[ex][1] * SIDE)
            sampled = product(
                tuple(t[rows] for t in turned), (wz_hi[:, lanes], wz_lo[:, lanes])
            )
            plain = sampled[:, :128]
            steep = sampled[:, 128:]
            total = jnp.concatenate(
                [
                    -jnp.sum(prod[col, 0, rows] * plain, axis=0, keepdims=True),
                    -jnp.sum(prod[col, 1, rows] * plain, axis=0, keepdims=True),
                    -jnp.sum(prod[col, 2, rows] * steep, axis=0, keepdims=True),
                    jnp.zeros((5, 128), F32),
                ],
                axis=0,
            )
            if ex >= 1 and ey >= 1:
                total = total + near[2 * ex + ey - 3] + SELF_GAIN * moving[it, ex, ey]
            part[ex, ey] = total

        for col in (0, 1, 2, 3, 6):
            gather(col)

        def last_copies():
            copies = []
            for k, (a, b) in enumerate(((1, 0), (0, 1), (1, 1))):
                span = {0: (1, 2), 1: (0, 1)}
                land = {0: (0, 2), 1: (0, 1)}
                copies.append(
                    pltpu.make_async_remote_copy(
                        src_ref=part.at[spans(span, a, b)],
                        dst_ref=last_in.at[(k, *spans(land, a, b))],
                        send_sem=part_send.at[k],
                        recv_sem=part_recv.at[k],
                        device_id=(wrap(mx - a), wrap(my - b)),
                        device_id_type=MESH,
                    )
                )
            return copies

        @pl.when(it == ITERS - 1)
        def _():
            for copy in last_copies():
                copy.start()

        for col in (4, 5, 7, 8):
            gather(col)

        @pl.when(it == 0)
        def _():
            copies = part_copies()
            for copy in copies:
                copy.start()
            for copy in copies:
                copy.wait()
            reach = {0: ((-1, 0), (0, 0)), 1: ((0, 1),), 2: ((0, 2), (1, 0)), 3: ((1, 1),)}
            for ex in range(4):
                for ey in range(4):
                    total = jnp.zeros((8, 128), F32)
                    for a, i in reach[ex]:
                        for b, j in reach[ey]:
                            if a == 0 and b == 0:
                                total = total + part[i, j]
                            else:
                                total = total + inbox[sides.index((a, b)), i, j]
                    moving[1, ex, ey] = fixed[ex, ey, 7:8] * (fixed[ex, ey, 8:16] + total)

        @pl.when(it == ITERS - 1)
        def _():
            for copy in last_copies():
                copy.wait()
            for cx in range(2):
                for cy in range(2):
                    total = part[cx + 1, cy + 1]
                    if cx == 1:
                        total = total + last_in[0, 0, cy]
                    if cy == 1:
                        total = total + last_in[1, cx, 0]
                    if cx == 1 and cy == 1:
                        total = total + last_in[2, 0, 0]
                    tile = fixed[cx + 1, cy + 1]
                    result = tile[7:8] * (tile[8:16] + total)
                    for c in range(3):
                        out[c, cx, cy : cy + 1] = result[c : c + 1]

        return carry

    lax.fori_loop(0, ITERS, iteration, 0)


def shards(cotangent, polarizability, site_offset, site_fraction, cell_count):
    vmem = pl.BlockSpec(memory_space=pltpu.VMEM)

    def room(*shape, dtype=F32):
        return pltpu.VMEM(shape, dtype)

    dma = pltpu.SemaphoreType.DMA
    return pl.pallas_call(
        kernel,
        out_shape=jax.ShapeDtypeStruct((3, 2, 2, 128), F32),
        in_specs=[pl.BlockSpec(memory_space=pl.ANY)] * 7,
        out_specs=vmem,
        scratch_shapes=[
            room(3, 2, 2, 128),
            room(2, 2, 128),
            room(3, 2, 2, 128, dtype=jnp.int32),
            room(3, 2, 2, 128),
            room(2, 2, 16, dtype=jnp.int32),
            room(2, 3 * N, N, dtype=BF16),
            room(4, HALF, N),
            room(4, 4, 16, 128),
            room(2, 4, 4, 8, 128),
            room(9, 3, N, 128),
            room(N, 9 * N, dtype=BF16),
            room(N, 9 * N, dtype=BF16),
            room(9 * N, N, dtype=BF16),
            room(9 * N, N, dtype=BF16),
            room(N, 9 * N, dtype=BF16),
            room(N, 9 * N, dtype=BF16),
            room(N, N),
            room(N, 2, 128),
            room(N, 2, 128),
            room(2, N, 2, 128),
            room(2, N, 2, 128),
            room(16, 3, 4, 8, 128),
            room(16, 3, 3, 8, 128),
            room(36, 3, 6, 8, 128),
            room(4, 8, 128),
            room(3, 3, 8, 128),
            room(8, 3, 3, 8, 128),
            room(3, 2, 2, 8, 128),
            dma((7,)),
            dma((4,)),
            dma((4,)),
            dma((2, 8)),
            dma((2, 8)),
            dma((3,)),
            dma((3,)),
            pltpu.SemaphoreType.REGULAR,
        ],
        compiler_params=pltpu.CompilerParams(
            collective_id=0, has_side_effects=True, vmem_limit_bytes=56 * 1024 * 1024
        ),
    )(
        cotangent,
        polarizability,
        site_offset,
        site_fraction,
        cell_count,
        *[jnp.asarray(table) for table in TABLES],
    )


def solution(mesh):
    return jax.shard_map(
        shards,
        mesh=mesh,
        in_specs=(
            P(None, "gx", "gy", None),
            P("gx", "gy", None),
            P(None, "gx", "gy", None),
            P(None, "gx", "gy", None),
            P("gx", "gy", None),
        ),
        out_specs=P(None, "gx", "gy", None),
        check_vma=False,
    )
```

```python
import math

import jax
import jax.numpy as jnp
import ml_dtypes
import numpy as np
from jax import lax
from jax.experimental import pallas as pl
from jax.experimental.pallas import tpu as pltpu
from jax.sharding import PartitionSpec as P

BETA = 0.7
THOLE = 0.39
ROOT_PI = 1.7724538509055159
SELF_GAIN = 4.0 * BETA * BETA * BETA / (3.0 * ROOT_PI)
ITERS = 2
N = 256
SIDE = 16
HALF = SIDE * (SIDE // 2 + 1)
MESH = pl.DeviceIdType.MESH
F32 = jnp.float32
BF16 = jnp.bfloat16

ERFC_P = (
    2.326819970068386e-2,
    -1.387039388740657e-1,
    3.687424674597105e-1,
    -5.824733027278666e-1,
    6.210004621745983e-1,
    -4.944515323274145e-1,
    3.404879937665872e-1,
    -2.741127028184656e-1,
    5.638259427386472e-1,
)
ERFC_R = (
    -1.047766399936249e1,
    1.297719955372516e1,
    -7.495518717768503e0,
    2.921019019210786e0,
    -1.015265279202700e0,
    4.218463358204948e-1,
    -2.820767439740514e-1,
    5.641895067754075e-1,
)
ERF_T = (
    7.853861353153693e-5,
    -8.010193625184903e-4,
    5.188327685732524e-3,
    -2.685381193529856e-2,
    1.128358514861418e-1,
    -3.761262582423300e-1,
    1.128379165726710e0,
)


def halves_np(table):
    high = table.astype(np.float32).astype(ml_dtypes.bfloat16)
    low = (table - high.astype(np.float64)).astype(np.float32).astype(ml_dtypes.bfloat16)
    return high, low


def tables():
    grid = np.arange(N)
    angle = 2.0 * math.pi / N * (grid[:, None] * grid[None, :] % N)
    hartley = np.cos(angle) + np.sin(angle)
    short = np.arange(SIDE)
    pair = (
        short[:, None, None, None] * short[None, None, :, None]
        + short[None, :, None, None] * short[None, None, None, :]
    ).reshape(N, N)
    outer = 2.0 * math.pi / SIDE * (pair % SIDE)
    twist = 2.0 * math.pi / N * (pair % N)

    def part(freq):
        signed = np.where(2 * freq < N, freq, freq - N) / N
        factor = 9.0 / (2.0 + np.cos(2.0 * math.pi * freq / N)) ** 2
        return signed * signed, factor

    low_x = short[:, None, None, None]
    low_y = short[None, :, None, None]
    freq_x = (low_x + SIDE * short[None, None, :, None]) + 0 * low_y
    freq_y = (low_y + SIDE * short[None, None, None, :]) + 0 * low_x
    square_x, factor_x = part(freq_x)
    square_y, factor_y = part(freq_y)
    square = (square_x + square_y).reshape(N, N)
    gain = (
        np.exp(-((math.pi / BETA) ** 2) * (square_x + square_y)) * factor_x * factor_y / math.pi
    ).reshape(N, N) / float(N * N * N)
    twice = np.where((grid // SIDE == 0) | (grid // SIDE == SIDE // 2), 1.0, 2.0)
    gain = gain * twice[:, None]
    waves = np.stack(halves_np(np.concatenate([hartley, np.cos(outer), -np.sin(outer)], axis=0)))
    plane = np.stack([np.cos(twist), -np.sin(twist), gain, square])[:, :HALF].astype(np.float32)
    return waves, plane


TABLES = tables()

SUPPORT = {0: (0, 3), 1: (0, 11), 2: (8, 16)}


def ring(offset, count):
    return min(offset, count - offset)


ROUTES = [
    (dy, dx, dz, dc)
    for dz in range(8)
    for dy in range(4)
    for dx in range(4)
    for dc in range(2)
    if (dy, dx, dz, dc) != (0, 0, 0, 0)
]


def order(route):
    across = ring(route[0], 4) + ring(route[1], 4)
    return -(across + ring(route[2], 8)), -across, route[0], route[1]


ROUTES.sort(key=order)

NN = (((1,), (0,)), ((), ()))
NT = (((1,), (1,)), ((), ()))


def halves(value):
    high = value.astype(BF16)
    return high, (value - high.astype(F32)).astype(BF16)


def product(left, right, dims=NN):
    def dot(a, b):
        return lax.dot_general(a, b, dims, preferred_element_type=F32)

    count = left[0].shape[0]
    both = dot(jnp.concatenate(left, axis=0), right[0])
    return both[:count] + (both[count:] + dot(left[0], right[1]))


def polynomial(terms, value):
    total = jnp.full_like(value, terms[0])
    for term in terms[1:]:
        total = total * value + term
    return total


def pair_coefficients(square, root):
    inverse = lax.rsqrt(square)
    distance = square * inverse
    inverse_square = 1.0 / square
    argument = BETA * distance
    steep = argument * argument
    bell = jnp.exp(-steep)
    ratio = inverse * (1.0 / BETA)
    small = ratio * ratio
    tail = jnp.where(
        argument < 2.0, polynomial(ERFC_P, small), polynomial(ERFC_R, small)
    )
    erfc = jnp.where(
        argument < 1.0,
        1.0 - argument * polynomial(ERF_T, steep),
        bell * ratio * tail,
    )
    gauss = (2.0 * BETA / ROOT_PI) * bell
    first = (erfc * inverse + gauss) * inverse_square
    second = (3.0 * first + (2.0 * BETA * BETA) * gauss) * inverse_square
    scaled = THOLE * square * distance * root
    damping = jnp.exp(-scaled)
    inverse_cube = inverse_square * inverse
    first = first - damping * inverse_cube
    second = second - 3.0 * (1.0 + scaled) * damping * inverse_cube * inverse_square
    return first, second


def spline(f):
    rest = 1.0 - f
    square = f * f
    cube = square * f
    values = (
        rest * rest * rest / 6.0,
        (3.0 * cube - 6.0 * square + 4.0) / 6.0,
        (-3.0 * cube + 3.0 * square + 3.0 * f + 1.0) / 6.0,
        cube / 6.0,
    )
    slopes = (
        -0.5 * rest * rest,
        0.5 * (3.0 * square - 4.0 * f),
        0.5 * (-3.0 * square + 2.0 * f + 1.0),
        0.5 * square,
    )
    return values, slopes


def placed(place, weights):
    total = jnp.where(place == 0, weights[0], 0.0)
    for order in range(1, 4):
        total = jnp.where(place == order, weights[order], total)
    return total


def kernel(
    cot_far, pol_far, off_far, frac_far, cnt_far, waves_far, plane_far,
    out,
    cot, pol, off, frac, cnt, waves, plane, fixed, moving, prod, wz_hi, wz_lo, wt_hi, wt_lo, p_hi, p_lo, spread,
    send_a, send_b, land_a, land_b, near_static, near_moving, tensor, near, part, inbox, last_in,
    table_sem, send_s, recv_s, halo_send, halo_recv, part_send, part_recv, second_level,
):
    mx = lax.axis_index("gx")
    my = lax.axis_index("gy")
    me = mx * SIDE + my

    def wrap(i):
        return lax.rem(i + SIDE, SIDE)

    arguments = [
        pltpu.make_async_copy(source, target, table_sem.at[2 + k])
        for k, (source, target) in enumerate(
            ((cot_far, cot), (pol_far, pol), (off_far, off), (frac_far, frac), (cnt_far, cnt))
        )
    ]
    table_copies = [
        pltpu.make_async_copy(waves_far, waves, table_sem.at[0]),
        pltpu.make_async_copy(plane_far, plane, table_sem.at[1]),
    ]
    for copy in arguments + table_copies:
        copy.start()

    entry = pltpu.get_barrier_semaphore()

    row_y, row_x, row_z = mx // 4, my // 8 * 2 + lax.rem(mx // 2, 2), lax.rem(my, 8)

    def place(dy, dx, dz, dc):
        to_y = lax.rem(row_y + dy, 4)
        to_x = lax.rem(row_x + dx, 4)
        to_core = lax.rem(mx + dc, 2)
        return (
            to_y * 4 + lax.rem(to_x, 2) * 2 + to_core,
            to_x // 2 * 8 + lax.rem(row_z + dz, 8),
        )

    sides = [(a, b) for a in (-1, 0, 1) for b in (-1, 0, 1) if (a, b) != (0, 0)]
    plane_peers = [r for r in ROUTES if r[2] == 0]
    line_peers = [r for r in ROUTES if r[:2] == (0, 0) and r[3] == 0]
    for route in plane_peers + line_peers:
        pl.semaphore_signal(entry, inc=1, device_id=place(*route), device_id_type=MESH)
    for a, b in sides:
        pl.semaphore_signal(
            entry, inc=1, device_id=(wrap(mx + a), wrap(my + b)), device_id_type=MESH
        )
    for copy in arguments:
        copy.wait()
    lane = lax.broadcasted_iota(jnp.int32, (8, 128), 1)
    row = lax.broadcasted_iota(jnp.int32, (8, 128), 0)
    expand = (
        lax.broadcasted_iota(jnp.int32, (16, 128), 1) // 8
        == lax.broadcasted_iota(jnp.int32, (16, 128), 0)
    ).astype(F32)
    slot = (lax.broadcasted_iota(jnp.int32, (2, 128), 1) % 8).astype(F32)
    for cx in range(2):
        counts = jnp.dot(cnt[cx].astype(F32), expand, preferred_element_type=F32)
        weight = jnp.where(slot < counts, 1.0, 0.0) * pol[cx]
        for cy in range(2):
            here = slice(cy, cy + 1)
            fixed[cx + 1, cy + 1] = jnp.concatenate(
                [off[c, cx, here].astype(F32) for c in range(3)]
                + [frac[c, cx, here] for c in range(3)]
                + [pol[cx, here], weight[here]]
                + [cot[c, cx, here] for c in range(3)]
                + [jnp.zeros((5, 128), F32)],
                axis=0,
            )

    pl.semaphore_wait(entry, len(plane_peers) + len(line_peers) + len(sides))

    def spans(table, a, b):
        return tuple(pl.ds(*table[side]) for side in (a, b))

    first_halo = []
    for k, (a, b) in enumerate(sides):
        first_halo.append(
            pltpu.make_async_remote_copy(
                src_ref=fixed.at[spans({-1: (1, 1), 0: (1, 2), 1: (2, 1)}, a, b)],
                dst_ref=fixed.at[spans({-1: (3, 1), 0: (1, 2), 1: (0, 1)}, a, b)],
                send_sem=halo_send.at[0, k],
                recv_sem=halo_recv.at[0, k],
                device_id=(wrap(mx + a), wrap(my + b)),
                device_id_type=MESH,
            )
        )
    for copy in first_halo:
        copy.start()
    for route in line_peers:
        pl.semaphore_signal(
            second_level, inc=1, device_id=place(*route), device_id_type=MESH
        )

    taken = {-1: (2, 1), 0: (0, 3), 1: (0, 2)}
    inner = {-1: (0, 1), 0: (0, 3), 1: (0, 2)}

    def part_copies():
        copies = []
        for a, b in sides:
            k = sides.index((-a, -b))
            copies.append(
                pltpu.make_async_remote_copy(
                    src_ref=part.at[spans(taken, -a, -b)],
                    dst_ref=inbox.at[(k, *spans(inner, -a, -b))],
                    send_sem=halo_send.at[1, k],
                    recv_sem=halo_recv.at[1, k],
                    device_id=(wrap(mx + a), wrap(my + b)),
                    device_id_type=MESH,
                )
            )
        return copies

    pick = [((lane // 8 + dz + 16) % 16) * 8 + row for dz in (-1, 0, 1)]

    def expanded(line, k):
        return jnp.take_along_axis(
            jnp.broadcast_to(line, (8, 128)), pick[k], axis=1, mode="promise_in_bounds"
        )

    def grow_static(col, carry):
        tile = fixed[col // 4, lax.rem(col, 4)]
        lines = [tile[c : c + 1] + 1.0 + tile[c + 3 : c + 4] for c in range(3)] + [tile[6:7]]
        for k in range(3):
            for c in range(4):
                value = expanded(lines[c], k)
                if c == 2:
                    value = value + 16.0 * (k - 1)
                near_static[col, k, c] = value
        return carry

    def grow_moving(it):
        def body(col, carry):
            tile = moving[it, col // 4, lax.rem(col, 4)]
            for k in range(3):
                for c in range(3):
                    near_moving[col, k, c] = expanded(tile[c : c + 1], k)
            return carry

        lax.fori_loop(0, 16, body, 0)

    tall = lax.broadcasted_iota(jnp.int32, (N, 128), 0)
    low = lax.broadcasted_iota(jnp.int32, (SIDE, 128), 0)
    cell_z = lax.broadcasted_iota(jnp.int32, (1, 128), 1) // 8 * 16

    def weights(ex, ey):
        col = ex * 3 + ey
        tile = fixed[ex, ey]
        anchor = tile[0:3].astype(jnp.int32)
        value, slope = zip(*[spline(tile[c + 3 : c + 4]) for c in range(3)])
        place_x = low - (anchor[0:1] + (ex - 1) * 8)
        place_y = low - (anchor[1:2] + (ey - 1) * 8)
        place_z = (tall - (anchor[2:3] + cell_z)) & (N - 1)
        wx, sx = placed(place_x, value[0]), placed(place_x, slope[0])
        wy, sy = placed(place_y, value[1]), placed(place_y, slope[1])
        for x in range(*SUPPORT[ex]):
            rows = pl.ds(x * SIDE, SIDE)
            prod[col, 0, rows] = sx[x : x + 1] * wy
            prod[col, 1, rows] = wx[x : x + 1] * sy
            prod[col, 2, rows] = wx[x : x + 1] * wy
        for k, source in enumerate((value[2], slope[2])):
            full = placed(place_z, source)
            lanes = pl.ds(pl.multiple_of(col * N + 128 * k, 128), 128)
            wz_hi[:, lanes], wz_lo[:, lanes] = halves(full)
            wt_hi[lanes, :], wt_lo[lanes, :] = halves(full.T)

    def weights_of(ex):
        def body(ey, carry):
            weights(ex, ey)
            return carry

        return body

    def spread_columns(it, groups, fresh):
        for ex, first, last in groups:
            rows = slice(SUPPORT[ex][0] * SIDE, SUPPORT[ex][1] * SIDE)
            for ey in range(first, last):
                col = 3 * ex + ey
                tile = moving[it, ex, ey]
                plain = tile[0:1] * prod[col, 0, rows] + tile[1:2] * prod[col, 1, rows]
                steep = tile[2:3] * prod[col, 2, rows]
                left = slice(col * N, col * N + 128)
                right = slice(col * N + 128, col * N + N)
                p_hi[rows, left], p_lo[rows, left] = halves(plain)
                p_hi[rows, right], p_lo[rows, right] = halves(steep)
            span = slice(N * (3 * ex + first), N * (3 * ex + last))
            term = product((p_hi[rows, span], p_lo[rows, span]), (wt_hi[span], wt_lo[span]))
            if fresh and ex == 1:
                spread[rows] = term
                spread[rows.stop :] = jnp.zeros((N - rows.stop, N), F32)
            else:
                spread[rows] += term

    def first_moment(ex, ey):
        tile = fixed[ex, ey]
        moving[0, ex, ey] = tile[7:8] * tile[8:16]

    owned = [(ex, ey) for ex in (1, 2) for ey in (1, 2)]
    for ex, ey in owned:
        first_moment(ex, ey)
    lax.fori_loop(1, 3, weights_of(1), 0)
    lax.fori_loop(1, 3, weights_of(2), 0)
    spread_columns(0, ((1, 1, 3), (2, 1, 3)), True)
    for copy in first_halo:
        copy.wait()
    for ex in range(4):
        for ey in range(4):
            if (ex, ey) not in owned:
                first_moment(ex, ey)
    for ey in range(3):
        weights(0, ey)
    weights(1, 0)
    weights(2, 0)
    spread_columns(0, ((1, 0, 1), (2, 0, 1), (0, 0, 3)), False)

    def pairs(item, carry):
        q = item // 9
        nb = lax.rem(item, 9)
        cx = q // 2
        cy = lax.rem(q, 2)
        dx = nb // 3 - 1
        dy = lax.rem(nb, 3) - 1
        tile = fixed[cx + 1, cy + 1]
        here = [tile[c : c + 1] + 1.0 + tile[c + 3 : c + 4] for c in range(3)]
        here[0] = here[0] - (8 * dx).astype(F32)
        here[1] = here[1] - (8 * dy).astype(F32)
        mine = tile[6:7]
        col = (cx + 1 + dx) * 4 + cy + 1 + dy
        for k in range(3):
            apart = [here[c] - near_static[col, k, c] for c in range(3)]
            square = apart[0] * apart[0] + apart[1] * apart[1] + apart[2] * apart[2]
            root = lax.rsqrt(mine * near_static[col, k, 3])
            if k == 1:
                same = (row == lane % 8) & (nb == 4)
                square = jnp.where(same, 1.0, square)
            c1, c2 = pair_coefficients(square, root)
            if k == 1:
                c1 = jnp.where(same, 0.0, c1)
                c2 = jnp.where(same, 0.0, c2)
            scaled = [c2 * apart[c] for c in range(3)]
            tensor[item, k, 0] = scaled[0] * apart[0] - c1
            tensor[item, k, 1] = scaled[1] * apart[1] - c1
            tensor[item, k, 2] = scaled[2] * apart[2] - c1
            tensor[item, k, 3] = scaled[0] * apart[1]
            tensor[item, k, 4] = scaled[0] * apart[2]
            tensor[item, k, 5] = scaled[1] * apart[2]
        return carry

    def near_field(it):
        grow_moving(it)

        def body(q, carry):
            cx = q // 2
            cy = lax.rem(q, 2)

            def inner(nb, total):
                fx, fy, fz = total
                col = (cx + nb // 3) * 4 + cy + lax.rem(nb, 3)
                item = q * 9 + nb
                for k in range(3):
                    vx, vy, vz = [near_moving[col, k, c] for c in range(3)]
                    xx, yy, zz, xy, xz, yz = [tensor[item, k, c] for c in range(6)]
                    fx = fx + (xx * vx + xy * vy + xz * vz)
                    fy = fy + (xy * vx + yy * vy + yz * vz)
                    fz = fz + (xz * vx + yz * vy + zz * vz)
                return fx, fy, fz

            zero = jnp.zeros((8, 128), F32)
            sums = lax.fori_loop(0, 9, inner, (zero, zero, zero))
            near[q] = jnp.concatenate(
                [jnp.sum(s, axis=0, keepdims=True) for s in sums]
                + [jnp.zeros((5, 128), F32)],
                axis=0,
            )
            return carry

        lax.fori_loop(0, 4, body, 0)

    def exchange(source, target, k):
        for route in ROUTES:
            gx, gy = place(*route)
            pltpu.make_async_remote_copy(
                src_ref=source.at[gx * SIDE + gy],
                dst_ref=target.at[me],
                send_sem=send_s.at[k],
                recv_sem=recv_s.at[k],
                device_id=(gx, gy),
                device_id_type=MESH,
            ).start()

        target[me] = source[me]

    def arrive(source, target, k):
        pltpu.make_async_remote_copy(
            src_ref=source.at[pl.ds(0, N - 1)],
            dst_ref=target.at[pl.ds(0, N - 1)],
            send_sem=send_s.at[k],
            recv_sem=recv_s.at[k],
            device_id=(mx, wrap(my + 1)),
            device_id_type=MESH,
        ).wait()

    def wave(k):
        return waves[0, N * k : N * (k + 1)], waves[1, N * k : N * (k + 1)]

    def put_rows(ref, value):
        ref[:, 0, :] = value[:, :128]
        ref[:, 1, :] = value[:, 128:]

    def get_rows(ref):
        return jnp.concatenate([ref[:, 0, :], ref[:, 1, :]], axis=1)

    def filtered(value):
        cosine = wave(1)
        sine = wave(2)
        upper = tuple(
            jnp.concatenate([c[:HALF], s[:HALF]], axis=0) for c, s in zip(cosine, sine)
        )
        both = product(upper, halves(value))
        re, im = both[:HALF], both[HALF:]
        tr, ti = plane[0], plane[1]
        both = halves(jnp.concatenate([re * tr - im * ti, re * ti + im * tr], axis=0))
        by_cosine = product(both, cosine)
        by_sine = product(both, sine)
        re = by_cosine[:HALF] - by_sine[HALF:]
        im = by_sine[:HALF] + by_cosine[HALF:]
        line = jnp.zeros((1, 128), F32) + me.astype(F32)
        signed = jnp.where(line < N // 2, line, line - N) * (1.0 / N)
        height = signed * signed
        bend = 2.0 + jnp.cos(line * (2.0 * math.pi / N))
        strength = jnp.exp(-((math.pi / BETA) ** 2) * height) * 9.0 / (bend * bend)
        height = jnp.concatenate([height, height], axis=1)
        strength = jnp.concatenate([strength, strength], axis=1)
        square = plane[3] + height
        centre = square == 0.0
        green = jnp.where(
            centre, 0.0, plane[2] * strength / jnp.where(centre, 1.0, square)
        )
        both = halves(jnp.concatenate([re * green, im * green], axis=0))
        by_cosine = product(both, cosine)
        by_sine = product(both, sine)
        re = by_cosine[:HALF] + by_sine[HALF:]
        im = by_cosine[HALF:] - by_sine[:HALF]
        first = halves(re * tr + im * ti)
        other = halves(im * tr - re * ti)
        cosine = tuple(c[:, :HALF] for c in cosine)
        sine = tuple(c[:, :HALF] for c in sine)
        return product(cosine, first) + product(sine, other)

    def iteration(it, carry):
        @pl.when(it > 0)
        def _():
            spread_columns(it, ((1, 0, 3), (2, 0, 3), (0, 0, 3)), True)

        @pl.when(it == 0)
        def _():
            for copy in table_copies:
                copy.wait()

        put_rows(send_a, product(wave(0), halves(spread[...]), NT))

        @pl.when(it == 0)
        def _():
            pl.semaphore_wait(second_level, len(line_peers))

        exchange(send_a, land_a.at[it], 2 * it)

        @pl.when(it == 0)
        def _():
            lax.fori_loop(0, 16, grow_static, 0)
            lax.fori_loop(0, 36, pairs, 0)

        arrive(send_a, land_a.at[it], 2 * it)
        put_rows(send_b, filtered(get_rows(land_a.at[it])))
        exchange(send_b, land_b.at[it], 2 * it + 1)
        near_field(it)
        arrive(send_b, land_b.at[it], 2 * it + 1)
        potential = product(wave(0), halves(get_rows(land_b.at[it])))
        turned = halves(potential.T)

        def gather(col):
            lanes = slice(col * N, col * N + N)
            ex, ey = col // 3, col % 3
            rows = slice(SUPPORT[ex][0] * SIDE, SUPPORT[ex][1] * SIDE)
            sampled = product(
                tuple(t[rows] for t in turned), (wz_hi[:, lanes], wz_lo[:, lanes])
            )
            plain = sampled[:, :128]
            steep = sampled[:, 128:]
            total = jnp.concatenate(
                [
                    -jnp.sum(prod[col, 0, rows] * plain, axis=0, keepdims=True),
                    -jnp.sum(prod[col, 1, rows] * plain, axis=0, keepdims=True),
                    -jnp.sum(prod[col, 2, rows] * steep, axis=0, keepdims=True),
                    jnp.zeros((5, 128), F32),
                ],
                axis=0,
            )
            if ex >= 1 and ey >= 1:
                total = total + near[2 * ex + ey - 3] + SELF_GAIN * moving[it, ex, ey]
            part[ex, ey] = total

        for col in (0, 1, 2, 3, 6):
            gather(col)

        def last_copies():
            copies = []
            for k, (a, b) in enumerate(((1, 0), (0, 1), (1, 1))):
                span = {0: (1, 2), 1: (0, 1)}
                land = {0: (0, 2), 1: (0, 1)}
                copies.append(
                    pltpu.make_async_remote_copy(
                        src_ref=part.at[spans(span, a, b)],
                        dst_ref=last_in.at[(k, *spans(land, a, b))],
                        send_sem=part_send.at[k],
                        recv_sem=part_recv.at[k],
                        device_id=(wrap(mx - a), wrap(my - b)),
                        device_id_type=MESH,
                    )
                )
            return copies

        @pl.when(it == ITERS - 1)
        def _():
            for copy in last_copies():
                copy.start()

        for col in (4, 5, 7, 8):
            gather(col)

        @pl.when(it == 0)
        def _():
            copies = part_copies()
            for copy in copies:
                copy.start()
            for copy in copies:
                copy.wait()
            reach = {0: ((-1, 0), (0, 0)), 1: ((0, 1),), 2: ((0, 2), (1, 0)), 3: ((1, 1),)}
            for ex in range(4):
                for ey in range(4):
                    total = jnp.zeros((8, 128), F32)
                    for a, i in reach[ex]:
                        for b, j in reach[ey]:
                            if a == 0 and b == 0:
                                total = total + part[i, j]
                            else:
                                total = total + inbox[sides.index((a, b)), i, j]
                    moving[1, ex, ey] = fixed[ex, ey, 7:8] * (fixed[ex, ey, 8:16] + total)

        @pl.when(it == ITERS - 1)
        def _():
            for copy in last_copies():
                copy.wait()
            for cx in range(2):
                for cy in range(2):
                    total = part[cx + 1, cy + 1]
                    if cx == 1:
                        total = total + last_in[0, 0, cy]
                    if cy == 1:
                        total = total + last_in[1, cx, 0]
                    if cx == 1 and cy == 1:
                        total = total + last_in[2, 0, 0]
                    tile = fixed[cx + 1, cy + 1]
                    result = tile[7:8] * (tile[8:16] + total)
                    for c in range(3):
                        out[c, cx, cy : cy + 1] = result[c : c + 1]

        return carry

    lax.fori_loop(0, ITERS, iteration, 0)


def shards(cotangent, polarizability, site_offset, site_fraction, cell_count):
    vmem = pl.BlockSpec(memory_space=pltpu.VMEM)

    def room(*shape, dtype=F32):
        return pltpu.VMEM(shape, dtype)

    dma = pltpu.SemaphoreType.DMA
    return pl.pallas_call(
        kernel,
        out_shape=jax.ShapeDtypeStruct((3, 2, 2, 128), F32),
        in_specs=[pl.BlockSpec(memory_space=pl.ANY)] * 7,
        out_specs=vmem,
        scratch_shapes=[
            room(3, 2, 2, 128),
            room(2, 2, 128),
            room(3, 2, 2, 128, dtype=jnp.int32),
            room(3, 2, 2, 128),
            room(2, 2, 16, dtype=jnp.int32),
            room(2, 3 * N, N, dtype=BF16),
            room(4, HALF, N),
            room(4, 4, 16, 128),
            room(2, 4, 4, 8, 128),
            room(9, 3, N, 128),
            room(N, 9 * N, dtype=BF16),
            room(N, 9 * N, dtype=BF16),
            room(9 * N, N, dtype=BF16),
            room(9 * N, N, dtype=BF16),
            room(N, 9 * N, dtype=BF16),
            room(N, 9 * N, dtype=BF16),
            room(N, N),
            room(N, 2, 128),
            room(N, 2, 128),
            room(2, N, 2, 128),
            room(2, N, 2, 128),
            room(16, 3, 4, 8, 128),
            room(16, 3, 3, 8, 128),
            room(36, 3, 6, 8, 128),
            room(4, 8, 128),
            room(3, 3, 8, 128),
            room(8, 3, 3, 8, 128),
            room(3, 2, 2, 8, 128),
            dma((7,)),
            dma((4,)),
            dma((4,)),
            dma((2, 8)),
            dma((2, 8)),
            dma((3,)),
            dma((3,)),
            pltpu.SemaphoreType.REGULAR,
        ],
        compiler_params=pltpu.CompilerParams(
            collective_id=0, has_side_effects=True, vmem_limit_bytes=56 * 1024 * 1024
        ),
    )(
        cotangent,
        polarizability,
        site_offset,
        site_fraction,
        cell_count,
        *[jnp.asarray(table) for table in TABLES],
    )


def solution(mesh):
    return jax.shard_map(
        shards,
        mesh=mesh,
        in_specs=(
            P(None, "gx", "gy", None),
            P("gx", "gy", None),
            P(None, "gx", "gy", None),
            P(None, "gx", "gy", None),
            P("gx", "gy", None),
        ),
        out_specs=P(None, "gx", "gy", None),
        check_vma=False,
    )
```

```python
import math

import jax
import jax.numpy as jnp
import ml_dtypes
import numpy as np
from jax import lax
from jax.experimental import pallas as pl
from jax.experimental.pallas import tpu as pltpu
from jax.sharding import PartitionSpec as P

BETA = 0.7
THOLE = 0.39
ROOT_PI = 1.7724538509055159
SELF_GAIN = 4.0 * BETA * BETA * BETA / (3.0 * ROOT_PI)
ITERS = 2
N = 256
SIDE = 16
HALF = SIDE * (SIDE // 2 + 1)
MESH = pl.DeviceIdType.MESH
F32 = jnp.float32
BF16 = jnp.bfloat16

ERFC_P = (
    2.326819970068386e-2,
    -1.387039388740657e-1,
    3.687424674597105e-1,
    -5.824733027278666e-1,
    6.210004621745983e-1,
    -4.944515323274145e-1,
    3.404879937665872e-1,
    -2.741127028184656e-1,
    5.638259427386472e-1,
)
ERFC_R = (
    -1.047766399936249e1,
    1.297719955372516e1,
    -7.495518717768503e0,
    2.921019019210786e0,
    -1.015265279202700e0,
    4.218463358204948e-1,
    -2.820767439740514e-1,
    5.641895067754075e-1,
)
ERF_T = (
    7.853861353153693e-5,
    -8.010193625184903e-4,
    5.188327685732524e-3,
    -2.685381193529856e-2,
    1.128358514861418e-1,
    -3.761262582423300e-1,
    1.128379165726710e0,
)


def halves_np(table):
    high = table.astype(np.float32).astype(ml_dtypes.bfloat16)
    low = (table - high.astype(np.float64)).astype(np.float32).astype(ml_dtypes.bfloat16)
    return high, low


def tables():
    grid = np.arange(N)
    angle = 2.0 * math.pi / N * (grid[:, None] * grid[None, :] % N)
    hartley = np.cos(angle) + np.sin(angle)
    short = np.arange(SIDE)
    pair = (
        short[:, None, None, None] * short[None, None, :, None]
        + short[None, :, None, None] * short[None, None, None, :]
    ).reshape(N, N)
    outer = 2.0 * math.pi / SIDE * (pair % SIDE)
    twist = 2.0 * math.pi / N * (pair % N)

    def part(freq):
        signed = np.where(2 * freq < N, freq, freq - N) / N
        factor = 9.0 / (2.0 + np.cos(2.0 * math.pi * freq / N)) ** 2
        return signed * signed, factor

    low_x = short[:, None, None, None]
    low_y = short[None, :, None, None]
    freq_x = (low_x + SIDE * short[None, None, :, None]) + 0 * low_y
    freq_y = (low_y + SIDE * short[None, None, None, :]) + 0 * low_x
    square_x, factor_x = part(freq_x)
    square_y, factor_y = part(freq_y)
    square = (square_x + square_y).reshape(N, N)
    gain = (
        np.exp(-((math.pi / BETA) ** 2) * (square_x + square_y)) * factor_x * factor_y / math.pi
    ).reshape(N, N) / float(N * N * N)
    twice = np.where((grid // SIDE == 0) | (grid // SIDE == SIDE // 2), 1.0, 2.0)
    gain = gain * twice[:, None]
    waves = np.stack(halves_np(np.concatenate([hartley, np.cos(outer), -np.sin(outer)], axis=0)))
    plane = np.stack([np.cos(twist), -np.sin(twist), gain, square])[:, :HALF].astype(np.float32)
    return waves, plane


TABLES = tables()

SUPPORT = {0: (0, 3), 1: (0, 11), 2: (8, 16)}


def ring(offset, count):
    return min(offset, count - offset)


ROUTES = [
    (dy, dx, dz, dc)
    for dz in range(8)
    for dy in range(4)
    for dx in range(4)
    for dc in range(2)
    if (dy, dx, dz, dc) != (0, 0, 0, 0)
]


def order(route):
    across = ring(route[0], 4) + ring(route[1], 4)
    return -(across + ring(route[2], 8)), -across, route[0], route[1]


ROUTES.sort(key=order)

NN = (((1,), (0,)), ((), ()))
NT = (((1,), (1,)), ((), ()))


def halves(value):
    high = value.astype(BF16)
    return high, (value - high.astype(F32)).astype(BF16)


def product(left, right, dims=NN):
    def dot(a, b):
        return lax.dot_general(a, b, dims, preferred_element_type=F32)

    count = left[0].shape[0]
    both = dot(jnp.concatenate(left, axis=0), right[0])
    return both[:count] + (both[count:] + dot(left[0], right[1]))


def polynomial(terms, value):
    total = jnp.full_like(value, terms[0])
    for term in terms[1:]:
        total = total * value + term
    return total


def pair_coefficients(square, root):
    inverse = lax.rsqrt(square)
    distance = square * inverse
    inverse_square = 1.0 / square
    argument = BETA * distance
    steep = argument * argument
    bell = jnp.exp(-steep)
    ratio = inverse * (1.0 / BETA)
    small = ratio * ratio
    tail = jnp.where(
        argument < 2.0, polynomial(ERFC_P, small), polynomial(ERFC_R, small)
    )
    erfc = jnp.where(
        argument < 1.0,
        1.0 - argument * polynomial(ERF_T, steep),
        bell * ratio * tail,
    )
    gauss = (2.0 * BETA / ROOT_PI) * bell
    first = (erfc * inverse + gauss) * inverse_square
    second = (3.0 * first + (2.0 * BETA * BETA) * gauss) * inverse_square
    scaled = THOLE * square * distance * root
    damping = jnp.exp(-scaled)
    inverse_cube = inverse_square * inverse
    first = first - damping * inverse_cube
    second = second - 3.0 * (1.0 + scaled) * damping * inverse_cube * inverse_square
    return first, second


def spline(f):
    rest = 1.0 - f
    square = f * f
    cube = square * f
    values = (
        rest * rest * rest / 6.0,
        (3.0 * cube - 6.0 * square + 4.0) / 6.0,
        (-3.0 * cube + 3.0 * square + 3.0 * f + 1.0) / 6.0,
        cube / 6.0,
    )
    slopes = (
        -0.5 * rest * rest,
        0.5 * (3.0 * square - 4.0 * f),
        0.5 * (-3.0 * square + 2.0 * f + 1.0),
        0.5 * square,
    )
    return values, slopes


def placed(place, weights):
    total = jnp.where(place == 0, weights[0], 0.0)
    for order in range(1, 4):
        total = jnp.where(place == order, weights[order], total)
    return total


def kernel(
    cot_far, pol_far, off_far, frac_far, cnt_far, waves_far, plane_far,
    out,
    cot, pol, off, frac, cnt, waves, plane, fixed, moving, prod, wz_hi, wz_lo, wt_hi, wt_lo, p_hi, p_lo, spread,
    send_a, send_b, land_a, land_b, near_static, near_moving, tensor, near, part, inbox, last_in,
    table_sem, send_s, recv_s, halo_send, halo_recv, part_send, part_recv, second_level,
):
    mx = lax.axis_index("gx")
    my = lax.axis_index("gy")
    me = mx * SIDE + my

    def wrap(i):
        return lax.rem(i + SIDE, SIDE)

    arguments = [
        pltpu.make_async_copy(source, target, table_sem.at[2 + k])
        for k, (source, target) in enumerate(
            ((cot_far, cot), (pol_far, pol), (off_far, off), (frac_far, frac), (cnt_far, cnt))
        )
    ]
    table_copies = [
        pltpu.make_async_copy(waves_far, waves, table_sem.at[0]),
        pltpu.make_async_copy(plane_far, plane, table_sem.at[1]),
    ]
    for copy in arguments + table_copies:
        copy.start()

    entry = pltpu.get_barrier_semaphore()

    row_y, row_x, row_z = mx // 4, my // 8 * 2 + lax.rem(mx // 2, 2), lax.rem(my, 8)

    def place(dy, dx, dz, dc):
        to_y = lax.rem(row_y + dy, 4)
        to_x = lax.rem(row_x + dx, 4)
        to_core = lax.rem(mx + dc, 2)
        return (
            to_y * 4 + lax.rem(to_x, 2) * 2 + to_core,
            to_x // 2 * 8 + lax.rem(row_z + dz, 8),
        )

    sides = [(a, b) for a in (-1, 0, 1) for b in (-1, 0, 1) if (a, b) != (0, 0)]
    plane_peers = [r for r in ROUTES if r[2] == 0]
    line_peers = [r for r in ROUTES if r[:2] == (0, 0) and r[3] == 0]
    for route in plane_peers + line_peers:
        pl.semaphore_signal(entry, inc=1, device_id=place(*route), device_id_type=MESH)
    for a, b in sides:
        pl.semaphore_signal(
            entry, inc=1, device_id=(wrap(mx + a), wrap(my + b)), device_id_type=MESH
        )
    for copy in arguments:
        copy.wait()
    lane = lax.broadcasted_iota(jnp.int32, (8, 128), 1)
    row = lax.broadcasted_iota(jnp.int32, (8, 128), 0)
    expand = (
        lax.broadcasted_iota(jnp.int32, (16, 128), 1) // 8
        == lax.broadcasted_iota(jnp.int32, (16, 128), 0)
    ).astype(F32)
    slot = (lax.broadcasted_iota(jnp.int32, (2, 128), 1) % 8).astype(F32)
    for cx in range(2):
        counts = jnp.dot(cnt[cx].astype(F32), expand, preferred_element_type=F32)
        weight = jnp.where(slot < counts, 1.0, 0.0) * pol[cx]
        for cy in range(2):
            here = slice(cy, cy + 1)
            fixed[cx + 1, cy + 1] = jnp.concatenate(
                [off[c, cx, here].astype(F32) for c in range(3)]
                + [frac[c, cx, here] for c in range(3)]
                + [pol[cx, here], weight[here]]
                + [cot[c, cx, here] for c in range(3)]
                + [jnp.zeros((5, 128), F32)],
                axis=0,
            )

    pl.semaphore_wait(entry, len(plane_peers) + len(line_peers) + len(sides))

    def spans(table, a, b):
        return tuple(pl.ds(*table[side]) for side in (a, b))

    first_halo = []
    for k, (a, b) in enumerate(sides):
        first_halo.append(
            pltpu.make_async_remote_copy(
                src_ref=fixed.at[spans({-1: (1, 1), 0: (1, 2), 1: (2, 1)}, a, b)],
                dst_ref=fixed.at[spans({-1: (3, 1), 0: (1, 2), 1: (0, 1)}, a, b)],
                send_sem=halo_send.at[0, k],
                recv_sem=halo_recv.at[0, k],
                device_id=(wrap(mx + a), wrap(my + b)),
                device_id_type=MESH,
            )
        )
    for copy in first_halo:
        copy.start()
    for route in line_peers:
        pl.semaphore_signal(
            second_level, inc=1, device_id=place(*route), device_id_type=MESH
        )

    taken = {-1: (2, 1), 0: (0, 3), 1: (0, 2)}
    inner = {-1: (0, 1), 0: (0, 3), 1: (0, 2)}

    def part_copies():
        copies = []
        for a, b in sides:
            k = sides.index((-a, -b))
            copies.append(
                pltpu.make_async_remote_copy(
                    src_ref=part.at[spans(taken, -a, -b)],
                    dst_ref=inbox.at[(k, *spans(inner, -a, -b))],
                    send_sem=halo_send.at[1, k],
                    recv_sem=halo_recv.at[1, k],
                    device_id=(wrap(mx + a), wrap(my + b)),
                    device_id_type=MESH,
                )
            )
        return copies

    pick = [((lane // 8 + dz + 16) % 16) * 8 + row for dz in (-1, 0, 1)]

    def expanded(line, k):
        return jnp.take_along_axis(
            jnp.broadcast_to(line, (8, 128)), pick[k], axis=1, mode="promise_in_bounds"
        )

    def grow_static(col, carry):
        tile = fixed[col // 4, lax.rem(col, 4)]
        lines = [tile[c : c + 1] + 1.0 + tile[c + 3 : c + 4] for c in range(3)] + [tile[6:7]]
        for k in range(3):
            for c in range(4):
                value = expanded(lines[c], k)
                if c == 2:
                    value = value + 16.0 * (k - 1)
                near_static[col, k, c] = value
        return carry

    def grow_moving(it):
        def body(col, carry):
            tile = moving[it, col // 4, lax.rem(col, 4)]
            for k in range(3):
                for c in range(3):
                    near_moving[col, k, c] = expanded(tile[c : c + 1], k)
            return carry

        lax.fori_loop(0, 16, body, 0)

    low = lax.broadcasted_iota(jnp.int32, (SIDE, 128), 0)
    cell_z = lax.broadcasted_iota(jnp.int32, (SIDE, 128), 1) // 8

    def weights(ex, ey):
        col = ex * 3 + ey
        tile = fixed[ex, ey]
        anchor = tile[0:3].astype(jnp.int32)
        value, slope = zip(*[spline(tile[c + 3 : c + 4]) for c in range(3)])
        place_x = low - (anchor[0:1] + (ex - 1) * 8)
        place_y = low - (anchor[1:2] + (ey - 1) * 8)
        place_z = low - anchor[2:3]
        wx, sx = placed(place_x, value[0]), placed(place_x, slope[0])
        wy, sy = placed(place_y, value[1]), placed(place_y, slope[1])
        for x in range(*SUPPORT[ex]):
            rows = pl.ds(x * SIDE, SIDE)
            prod[col, 0, rows] = sx[x : x + 1] * wy
            prod[col, 1, rows] = wx[x : x + 1] * sy
            prod[col, 2, rows] = wx[x : x + 1] * wy
        for k, source in enumerate((value[2], slope[2])):
            base = placed(place_z, source)
            spill = placed(place_z + SIDE, source)
            full = jnp.concatenate(
                [
                    jnp.where(
                        cell_z == cell,
                        base,
                        jnp.where(cell_z == (cell + SIDE - 1) % SIDE, spill, 0.0),
                    )
                    for cell in range(SIDE)
                ],
                axis=0,
            )
            lanes = pl.ds(pl.multiple_of(col * N + 128 * k, 128), 128)
            wz_hi[:, lanes], wz_lo[:, lanes] = halves(full)
            wt_hi[lanes, :], wt_lo[lanes, :] = halves(full.T)

    def weights_of(ex):
        def body(ey, carry):
            weights(ex, ey)
            return carry

        return body

    def spread_columns(it, groups, fresh):
        for ex, first, last in groups:
            rows = slice(SUPPORT[ex][0] * SIDE, SUPPORT[ex][1] * SIDE)
            for ey in range(first, last):
                col = 3 * ex + ey
                tile = moving[it, ex, ey]
                plain = tile[0:1] * prod[col, 0, rows] + tile[1:2] * prod[col, 1, rows]
                steep = tile[2:3] * prod[col, 2, rows]
                left = slice(col * N, col * N + 128)
                right = slice(col * N + 128, col * N + N)
                p_hi[rows, left], p_lo[rows, left] = halves(plain)
                p_hi[rows, right], p_lo[rows, right] = halves(steep)
            span = slice(N * (3 * ex + first), N * (3 * ex + last))
            term = product((p_hi[rows, span], p_lo[rows, span]), (wt_hi[span], wt_lo[span]))
            if fresh and ex == 1:
                spread[rows] = term
                spread[rows.stop :] = jnp.zeros((N - rows.stop, N), F32)
            else:
                spread[rows] += term

    def first_moment(ex, ey):
        tile = fixed[ex, ey]
        moving[0, ex, ey] = tile[7:8] * tile[8:16]

    owned = [(ex, ey) for ex in (1, 2) for ey in (1, 2)]
    for ex, ey in owned:
        first_moment(ex, ey)
    lax.fori_loop(1, 3, weights_of(1), 0)
    lax.fori_loop(1, 3, weights_of(2), 0)
    spread_columns(0, ((1, 1, 3), (2, 1, 3)), True)
    for copy in first_halo:
        copy.wait()
    for ex in range(4):
        for ey in range(4):
            if (ex, ey) not in owned:
                first_moment(ex, ey)
    for ey in range(3):
        weights(0, ey)
    weights(1, 0)
    weights(2, 0)
    spread_columns(0, ((1, 0, 1), (2, 0, 1), (0, 0, 3)), False)

    def pairs(item, carry):
        q = item // 9
        nb = lax.rem(item, 9)
        cx = q // 2
        cy = lax.rem(q, 2)
        dx = nb // 3 - 1
        dy = lax.rem(nb, 3) - 1
        tile = fixed[cx + 1, cy + 1]
        here = [tile[c : c + 1] + 1.0 + tile[c + 3 : c + 4] for c in range(3)]
        here[0] = here[0] - (8 * dx).astype(F32)
        here[1] = here[1] - (8 * dy).astype(F32)
        mine = tile[6:7]
        col = (cx + 1 + dx) * 4 + cy + 1 + dy
        for k in range(3):
            apart = [here[c] - near_static[col, k, c] for c in range(3)]
            square = apart[0] * apart[0] + apart[1] * apart[1] + apart[2] * apart[2]
            root = lax.rsqrt(mine * near_static[col, k, 3])
            if k == 1:
                same = (row == lane % 8) & (nb == 4)
                square = jnp.where(same, 1.0, square)
            c1, c2 = pair_coefficients(square, root)
            if k == 1:
                c1 = jnp.where(same, 0.0, c1)
                c2 = jnp.where(same, 0.0, c2)
            scaled = [c2 * apart[c] for c in range(3)]
            tensor[item, k, 0] = scaled[0] * apart[0] - c1
            tensor[item, k, 1] = scaled[1] * apart[1] - c1
            tensor[item, k, 2] = scaled[2] * apart[2] - c1
            tensor[item, k, 3] = scaled[0] * apart[1]
            tensor[item, k, 4] = scaled[0] * apart[2]
            tensor[item, k, 5] = scaled[1] * apart[2]
        return carry

    def near_field(it):
        grow_moving(it)

        def body(q, carry):
            cx = q // 2
            cy = lax.rem(q, 2)

            def inner(nb, total):
                fx, fy, fz = total
                col = (cx + nb // 3) * 4 + cy + lax.rem(nb, 3)
                item = q * 9 + nb
                for k in range(3):
                    vx, vy, vz = [near_moving[col, k, c] for c in range(3)]
                    xx, yy, zz, xy, xz, yz = [tensor[item, k, c] for c in range(6)]
                    fx = fx + (xx * vx + xy * vy + xz * vz)
                    fy = fy + (xy * vx + yy * vy + yz * vz)
                    fz = fz + (xz * vx + yz * vy + zz * vz)
                return fx, fy, fz

            zero = jnp.zeros((8, 128), F32)
            sums = lax.fori_loop(0, 9, inner, (zero, zero, zero))
            near[q] = jnp.concatenate(
                [jnp.sum(s, axis=0, keepdims=True) for s in sums]
                + [jnp.zeros((5, 128), F32)],
                axis=0,
            )
            return carry

        lax.fori_loop(0, 4, body, 0)

    def exchange(source, target, k):
        for route in ROUTES:
            gx, gy = place(*route)
            pltpu.make_async_remote_copy(
                src_ref=source.at[gx * SIDE + gy],
                dst_ref=target.at[me],
                send_sem=send_s.at[k],
                recv_sem=recv_s.at[k],
                device_id=(gx, gy),
                device_id_type=MESH,
            ).start()

        target[me] = source[me]

    def arrive(source, target, k):
        pltpu.make_async_remote_copy(
            src_ref=source.at[pl.ds(0, N - 1)],
            dst_ref=target.at[pl.ds(0, N - 1)],
            send_sem=send_s.at[k],
            recv_sem=recv_s.at[k],
            device_id=(mx, wrap(my + 1)),
            device_id_type=MESH,
        ).wait()

    def wave(k):
        return waves[0, N * k : N * (k + 1)], waves[1, N * k : N * (k + 1)]

    def put_rows(ref, value):
        ref[:, 0, :] = value[:, :128]
        ref[:, 1, :] = value[:, 128:]

    def get_rows(ref):
        return jnp.concatenate([ref[:, 0, :], ref[:, 1, :]], axis=1)

    def filtered(value):
        cosine = wave(1)
        sine = wave(2)
        upper = tuple(
            jnp.concatenate([c[:HALF], s[:HALF]], axis=0) for c, s in zip(cosine, sine)
        )
        both = product(upper, halves(value))
        re, im = both[:HALF], both[HALF:]
        tr, ti = plane[0], plane[1]
        both = halves(jnp.concatenate([re * tr - im * ti, re * ti + im * tr], axis=0))
        by_cosine = product(both, cosine)
        by_sine = product(both, sine)
        re = by_cosine[:HALF] - by_sine[HALF:]
        im = by_sine[:HALF] + by_cosine[HALF:]
        line = jnp.zeros((1, 128), F32) + me.astype(F32)
        signed = jnp.where(line < N // 2, line, line - N) * (1.0 / N)
        height = signed * signed
        bend = 2.0 + jnp.cos(line * (2.0 * math.pi / N))
        strength = jnp.exp(-((math.pi / BETA) ** 2) * height) * 9.0 / (bend * bend)
        height = jnp.concatenate([height, height], axis=1)
        strength = jnp.concatenate([strength, strength], axis=1)
        square = plane[3] + height
        centre = square == 0.0
        green = jnp.where(
            centre, 0.0, plane[2] * strength / jnp.where(centre, 1.0, square)
        )
        both = halves(jnp.concatenate([re * green, im * green], axis=0))
        by_cosine = product(both, cosine)
        by_sine = product(both, sine)
        re = by_cosine[:HALF] + by_sine[HALF:]
        im = by_cosine[HALF:] - by_sine[:HALF]
        first = halves(re * tr + im * ti)
        other = halves(im * tr - re * ti)
        cosine = tuple(c[:, :HALF] for c in cosine)
        sine = tuple(c[:, :HALF] for c in sine)
        return product(cosine, first) + product(sine, other)

    def iteration(it, carry):
        @pl.when(it > 0)
        def _():
            spread_columns(it, ((1, 0, 3), (2, 0, 3), (0, 0, 3)), True)

        @pl.when(it == 0)
        def _():
            for copy in table_copies:
                copy.wait()

        put_rows(send_a, product(wave(0), halves(spread[...]), NT))

        @pl.when(it == 0)
        def _():
            pl.semaphore_wait(second_level, len(line_peers))

        exchange(send_a, land_a.at[it], 2 * it)

        @pl.when(it == 0)
        def _():
            lax.fori_loop(0, 16, grow_static, 0)
            lax.fori_loop(0, 36, pairs, 0)

        arrive(send_a, land_a.at[it], 2 * it)
        put_rows(send_b, filtered(get_rows(land_a.at[it])))
        exchange(send_b, land_b.at[it], 2 * it + 1)
        near_field(it)

        @pl.when(it == 0)
        def _():
            def fold(col, carry):
                lanes = pl.ds(pl.multiple_of(col * N, N), N)
                wz_hi[:, lanes], wz_lo[:, lanes] = halves(
                    product(wave(0), (wz_hi[:, lanes], wz_lo[:, lanes]))
                )
                return carry

            lax.fori_loop(0, 9, fold, 0)

        arrive(send_b, land_b.at[it], 2 * it + 1)
        turned = halves(get_rows(land_b.at[it]).T)

        def gather(col):
            lanes = slice(col * N, col * N + N)
            ex, ey = col // 3, col % 3
            rows = slice(SUPPORT[ex][0] * SIDE, SUPPORT[ex][1] * SIDE)
            sampled = product(
                tuple(t[rows] for t in turned), (wz_hi[:, lanes], wz_lo[:, lanes])
            )
            plain = sampled[:, :128]
            steep = sampled[:, 128:]
            total = jnp.concatenate(
                [
                    -jnp.sum(prod[col, 0, rows] * plain, axis=0, keepdims=True),
                    -jnp.sum(prod[col, 1, rows] * plain, axis=0, keepdims=True),
                    -jnp.sum(prod[col, 2, rows] * steep, axis=0, keepdims=True),
                    jnp.zeros((5, 128), F32),
                ],
                axis=0,
            )
            if ex >= 1 and ey >= 1:
                total = total + near[2 * ex + ey - 3] + SELF_GAIN * moving[it, ex, ey]
            part[ex, ey] = total

        for col in (0, 1, 2, 3, 6):
            gather(col)

        def last_copies():
            copies = []
            for k, (a, b) in enumerate(((1, 0), (0, 1), (1, 1))):
                span = {0: (1, 2), 1: (0, 1)}
                land = {0: (0, 2), 1: (0, 1)}
                copies.append(
                    pltpu.make_async_remote_copy(
                        src_ref=part.at[spans(span, a, b)],
                        dst_ref=last_in.at[(k, *spans(land, a, b))],
                        send_sem=part_send.at[k],
                        recv_sem=part_recv.at[k],
                        device_id=(wrap(mx - a), wrap(my - b)),
                        device_id_type=MESH,
                    )
                )
            return copies

        @pl.when(it == ITERS - 1)
        def _():
            for copy in last_copies():
                copy.start()

        for col in (4, 5, 7, 8):
            gather(col)

        @pl.when(it == 0)
        def _():
            copies = part_copies()
            for copy in copies:
                copy.start()
            for copy in copies:
                copy.wait()
            reach = {0: ((-1, 0), (0, 0)), 1: ((0, 1),), 2: ((0, 2), (1, 0)), 3: ((1, 1),)}
            for ex in range(4):
                for ey in range(4):
                    total = jnp.zeros((8, 128), F32)
                    for a, i in reach[ex]:
                        for b, j in reach[ey]:
                            if a == 0 and b == 0:
                                total = total + part[i, j]
                            else:
                                total = total + inbox[sides.index((a, b)), i, j]
                    moving[1, ex, ey] = fixed[ex, ey, 7:8] * (fixed[ex, ey, 8:16] + total)

        @pl.when(it == ITERS - 1)
        def _():
            for copy in last_copies():
                copy.wait()
            for cx in range(2):
                for cy in range(2):
                    total = part[cx + 1, cy + 1]
                    if cx == 1:
                        total = total + last_in[0, 0, cy]
                    if cy == 1:
                        total = total + last_in[1, cx, 0]
                    if cx == 1 and cy == 1:
                        total = total + last_in[2, 0, 0]
                    tile = fixed[cx + 1, cy + 1]
                    result = tile[7:8] * (tile[8:16] + total)
                    for c in range(3):
                        out[c, cx, cy : cy + 1] = result[c : c + 1]

        return carry

    lax.fori_loop(0, ITERS, iteration, 0)


def shards(cotangent, polarizability, site_offset, site_fraction, cell_count):
    vmem = pl.BlockSpec(memory_space=pltpu.VMEM)

    def room(*shape, dtype=F32):
        return pltpu.VMEM(shape, dtype)

    dma = pltpu.SemaphoreType.DMA
    return pl.pallas_call(
        kernel,
        out_shape=jax.ShapeDtypeStruct((3, 2, 2, 128), F32),
        in_specs=[pl.BlockSpec(memory_space=pl.ANY)] * 7,
        out_specs=vmem,
        scratch_shapes=[
            room(3, 2, 2, 128),
            room(2, 2, 128),
            room(3, 2, 2, 128, dtype=jnp.int32),
            room(3, 2, 2, 128),
            room(2, 2, 16, dtype=jnp.int32),
            room(2, 3 * N, N, dtype=BF16),
            room(4, HALF, N),
            room(4, 4, 16, 128),
            room(2, 4, 4, 8, 128),
            room(9, 3, N, 128),
            room(N, 9 * N, dtype=BF16),
            room(N, 9 * N, dtype=BF16),
            room(9 * N, N, dtype=BF16),
            room(9 * N, N, dtype=BF16),
            room(N, 9 * N, dtype=BF16),
            room(N, 9 * N, dtype=BF16),
            room(N, N),
            room(N, 2, 128),
            room(N, 2, 128),
            room(2, N, 2, 128),
            room(2, N, 2, 128),
            room(16, 3, 4, 8, 128),
            room(16, 3, 3, 8, 128),
            room(36, 3, 6, 8, 128),
            room(4, 8, 128),
            room(3, 3, 8, 128),
            room(8, 3, 3, 8, 128),
            room(3, 2, 2, 8, 128),
            dma((7,)),
            dma((4,)),
            dma((4,)),
            dma((2, 8)),
            dma((2, 8)),
            dma((3,)),
            dma((3,)),
            pltpu.SemaphoreType.REGULAR,
        ],
        compiler_params=pltpu.CompilerParams(
            collective_id=0, has_side_effects=True, vmem_limit_bytes=56 * 1024 * 1024
        ),
    )(
        cotangent,
        polarizability,
        site_offset,
        site_fraction,
        cell_count,
        *[jnp.asarray(table) for table in TABLES],
    )


def solution(mesh):
    return jax.shard_map(
        shards,
        mesh=mesh,
        in_specs=(
            P(None, "gx", "gy", None),
            P("gx", "gy", None),
            P(None, "gx", "gy", None),
            P(None, "gx", "gy", None),
            P("gx", "gy", None),
        ),
        out_specs=P(None, "gx", "gy", None),
        check_vma=False,
    )
```

```python
import math

import jax
import jax.numpy as jnp
import ml_dtypes
import numpy as np
from jax import lax
from jax.experimental import pallas as pl
from jax.experimental.pallas import tpu as pltpu
from jax.sharding import PartitionSpec as P

BETA = 0.7
THOLE = 0.39
ROOT_PI = 1.7724538509055159
SELF_GAIN = 4.0 * BETA * BETA * BETA / (3.0 * ROOT_PI)
ITERS = 2
N = 256
SIDE = 16
HALF = SIDE * (SIDE // 2 + 1)
MESH = pl.DeviceIdType.MESH
F32 = jnp.float32
BF16 = jnp.bfloat16

ERFC_P = (
    2.326819970068386e-2,
    -1.387039388740657e-1,
    3.687424674597105e-1,
    -5.824733027278666e-1,
    6.210004621745983e-1,
    -4.944515323274145e-1,
    3.404879937665872e-1,
    -2.741127028184656e-1,
    5.638259427386472e-1,
)
ERFC_R = (
    -1.047766399936249e1,
    1.297719955372516e1,
    -7.495518717768503e0,
    2.921019019210786e0,
    -1.015265279202700e0,
    4.218463358204948e-1,
    -2.820767439740514e-1,
    5.641895067754075e-1,
)
ERF_T = (
    7.853861353153693e-5,
    -8.010193625184903e-4,
    5.188327685732524e-3,
    -2.685381193529856e-2,
    1.128358514861418e-1,
    -3.761262582423300e-1,
    1.128379165726710e0,
)


def halves_np(table):
    high = table.astype(np.float32).astype(ml_dtypes.bfloat16)
    low = (table - high.astype(np.float64)).astype(np.float32).astype(ml_dtypes.bfloat16)
    return high, low


def tables():
    grid = np.arange(N)
    angle = 2.0 * math.pi / N * (grid[:, None] * grid[None, :] % N)
    hartley = np.cos(angle) + np.sin(angle)
    short = np.arange(SIDE)
    pair = (
        short[:, None, None, None] * short[None, None, :, None]
        + short[None, :, None, None] * short[None, None, None, :]
    ).reshape(N, N)
    outer = 2.0 * math.pi / SIDE * (pair % SIDE)
    twist = 2.0 * math.pi / N * (pair % N)

    def part(freq):
        signed = np.where(2 * freq < N, freq, freq - N) / N
        factor = 9.0 / (2.0 + np.cos(2.0 * math.pi * freq / N)) ** 2
        return signed * signed, factor

    low_x = short[:, None, None, None]
    low_y = short[None, :, None, None]
    freq_x = (low_x + SIDE * short[None, None, :, None]) + 0 * low_y
    freq_y = (low_y + SIDE * short[None, None, None, :]) + 0 * low_x
    square_x, factor_x = part(freq_x)
    square_y, factor_y = part(freq_y)
    square = (square_x + square_y).reshape(N, N)
    gain = (
        np.exp(-((math.pi / BETA) ** 2) * (square_x + square_y)) * factor_x * factor_y / math.pi
    ).reshape(N, N) / float(N * N * N)
    twice = np.where((grid // SIDE == 0) | (grid // SIDE == SIDE // 2), 1.0, 2.0)
    gain = gain * twice[:, None]
    waves = np.stack(halves_np(np.concatenate([hartley, np.cos(outer), -np.sin(outer)], axis=0)))
    plane = np.stack([np.cos(twist), -np.sin(twist), gain, square])[:, :HALF].astype(np.float32)
    return waves, plane


TABLES = tables()

SUPPORT = {0: (0, 3), 1: (0, 11), 2: (8, 16)}


def ring(offset, count):
    return min(offset, count - offset)


ROUTES = [
    (dy, dx, dz, dc)
    for dz in range(8)
    for dy in range(4)
    for dx in range(4)
    for dc in range(2)
    if (dy, dx, dz, dc) != (0, 0, 0, 0)
]


def order(route):
    across = ring(route[0], 4) + ring(route[1], 4)
    return -(across + ring(route[2], 8)), -across, route[0], route[1]


ROUTES.sort(key=order)

NN = (((1,), (0,)), ((), ()))
NT = (((1,), (1,)), ((), ()))


def halves(value):
    high = value.astype(BF16)
    return high, (value - high.astype(F32)).astype(BF16)


def product(left, right, dims=NN):
    def dot(a, b):
        return lax.dot_general(a, b, dims, preferred_element_type=F32)

    count = left[0].shape[0]
    both = dot(jnp.concatenate(left, axis=0), right[0])
    return both[:count] + (both[count:] + dot(left[0], right[1]))


def polynomial(terms, value):
    total = jnp.full_like(value, terms[0])
    for term in terms[1:]:
        total = total * value + term
    return total


def pair_coefficients(square, root):
    inverse = lax.rsqrt(square)
    distance = square * inverse
    inverse_square = 1.0 / square
    argument = BETA * distance
    steep = argument * argument
    bell = jnp.exp(-steep)
    ratio = inverse * (1.0 / BETA)
    small = ratio * ratio
    tail = jnp.where(
        argument < 2.0, polynomial(ERFC_P, small), polynomial(ERFC_R, small)
    )
    erfc = jnp.where(
        argument < 1.0,
        1.0 - argument * polynomial(ERF_T, steep),
        bell * ratio * tail,
    )
    gauss = (2.0 * BETA / ROOT_PI) * bell
    first = (erfc * inverse + gauss) * inverse_square
    second = (3.0 * first + (2.0 * BETA * BETA) * gauss) * inverse_square
    scaled = THOLE * square * distance * root
    damping = jnp.exp(-scaled)
    inverse_cube = inverse_square * inverse
    first = first - damping * inverse_cube
    second = second - 3.0 * (1.0 + scaled) * damping * inverse_cube * inverse_square
    return first, second


def spline(f):
    rest = 1.0 - f
    square = f * f
    cube = square * f
    values = (
        rest * rest * rest / 6.0,
        (3.0 * cube - 6.0 * square + 4.0) / 6.0,
        (-3.0 * cube + 3.0 * square + 3.0 * f + 1.0) / 6.0,
        cube / 6.0,
    )
    slopes = (
        -0.5 * rest * rest,
        0.5 * (3.0 * square - 4.0 * f),
        0.5 * (-3.0 * square + 2.0 * f + 1.0),
        0.5 * square,
    )
    return values, slopes


def placed(place, weights):
    total = jnp.where(place == 0, weights[0], 0.0)
    for order in range(1, 4):
        total = jnp.where(place == order, weights[order], total)
    return total


def kernel(
    cot_far, pol_far, off_far, frac_far, cnt_far, waves_far, plane_far,
    out,
    cot, pol, off, frac, cnt, waves, plane, fixed, moving, prod, wz_hi, wz_lo, wt_hi, wt_lo, p_hi, p_lo, spread,
    send_a, send_b, land_a, land_b, near_static, near_moving, tensor, near, part, inbox, last_in,
    table_sem, send_s, recv_s, halo_send, halo_recv, part_send, part_recv, second_level,
):
    mx = lax.axis_index("gx")
    my = lax.axis_index("gy")
    me = mx * SIDE + my

    def wrap(i):
        return lax.rem(i + SIDE, SIDE)

    arguments = [
        pltpu.make_async_copy(source, target, table_sem.at[2 + k])
        for k, (source, target) in enumerate(
            ((cot_far, cot), (pol_far, pol), (off_far, off), (frac_far, frac), (cnt_far, cnt))
        )
    ]
    table_copies = [
        pltpu.make_async_copy(waves_far, waves, table_sem.at[0]),
        pltpu.make_async_copy(plane_far, plane, table_sem.at[1]),
    ]
    for copy in arguments + table_copies:
        copy.start()

    entry = pltpu.get_barrier_semaphore()

    row_y, row_x, row_z = mx // 4, my // 8 * 2 + lax.rem(mx // 2, 2), lax.rem(my, 8)

    def place(dy, dx, dz, dc):
        to_y = lax.rem(row_y + dy, 4)
        to_x = lax.rem(row_x + dx, 4)
        to_core = lax.rem(mx + dc, 2)
        return (
            to_y * 4 + lax.rem(to_x, 2) * 2 + to_core,
            to_x // 2 * 8 + lax.rem(row_z + dz, 8),
        )

    sides = [(a, b) for a in (-1, 0, 1) for b in (-1, 0, 1) if (a, b) != (0, 0)]
    plane_peers = [r for r in ROUTES if r[2] == 0]
    line_peers = [r for r in ROUTES if r[:2] == (0, 0) and r[3] == 0]
    for route in plane_peers + line_peers:
        pl.semaphore_signal(entry, inc=1, device_id=place(*route), device_id_type=MESH)
    for a, b in sides:
        pl.semaphore_signal(
            entry, inc=1, device_id=(wrap(mx + a), wrap(my + b)), device_id_type=MESH
        )
    for copy in arguments:
        copy.wait()
    lane = lax.broadcasted_iota(jnp.int32, (8, 128), 1)
    row = lax.broadcasted_iota(jnp.int32, (8, 128), 0)
    expand = (
        lax.broadcasted_iota(jnp.int32, (16, 128), 1) // 8
        == lax.broadcasted_iota(jnp.int32, (16, 128), 0)
    ).astype(F32)
    slot = (lax.broadcasted_iota(jnp.int32, (2, 128), 1) % 8).astype(F32)
    for cx in range(2):
        counts = jnp.dot(cnt[cx].astype(F32), expand, preferred_element_type=F32)
        weight = jnp.where(slot < counts, 1.0, 0.0) * pol[cx]
        for cy in range(2):
            here = slice(cy, cy + 1)
            fixed[cx + 1, cy + 1] = jnp.concatenate(
                [off[c, cx, here].astype(F32) for c in range(3)]
                + [frac[c, cx, here] for c in range(3)]
                + [pol[cx, here], weight[here]]
                + [cot[c, cx, here] for c in range(3)]
                + [jnp.zeros((5, 128), F32)],
                axis=0,
            )

    pl.semaphore_wait(entry, len(plane_peers) + len(line_peers) + len(sides))

    def spans(table, a, b):
        return tuple(pl.ds(*table[side]) for side in (a, b))

    first_halo = []
    for k, (a, b) in enumerate(sides):
        first_halo.append(
            pltpu.make_async_remote_copy(
                src_ref=fixed.at[spans({-1: (1, 1), 0: (1, 2), 1: (2, 1)}, a, b)],
                dst_ref=fixed.at[spans({-1: (3, 1), 0: (1, 2), 1: (0, 1)}, a, b)],
                send_sem=halo_send.at[0, k],
                recv_sem=halo_recv.at[0, k],
                device_id=(wrap(mx + a), wrap(my + b)),
                device_id_type=MESH,
            )
        )
    for copy in first_halo:
        copy.start()
    for route in line_peers:
        pl.semaphore_signal(
            second_level, inc=1, device_id=place(*route), device_id_type=MESH
        )

    taken = {-1: (2, 1), 0: (0, 3), 1: (0, 2)}
    inner = {-1: (0, 1), 0: (0, 3), 1: (0, 2)}

    def part_copies():
        copies = []
        for a, b in sides:
            k = sides.index((-a, -b))
            copies.append(
                pltpu.make_async_remote_copy(
                    src_ref=part.at[spans(taken, -a, -b)],
                    dst_ref=inbox.at[(k, *spans(inner, -a, -b))],
                    send_sem=halo_send.at[1, k],
                    recv_sem=halo_recv.at[1, k],
                    device_id=(wrap(mx + a), wrap(my + b)),
                    device_id_type=MESH,
                )
            )
        return copies

    pick = [((lane // 8 + dz + 16) % 16) * 8 + row for dz in (-1, 0, 1)]

    def expanded(line, k):
        return jnp.take_along_axis(
            jnp.broadcast_to(line, (8, 128)), pick[k], axis=1, mode="promise_in_bounds"
        )

    def grow_static(col, carry):
        tile = fixed[col // 4, lax.rem(col, 4)]
        lines = [tile[c : c + 1] + 1.0 + tile[c + 3 : c + 4] for c in range(3)] + [tile[6:7]]
        for k in range(3):
            for c in range(4):
                value = expanded(lines[c], k)
                if c == 2:
                    value = value + 16.0 * (k - 1)
                near_static[col, k, c] = value
        return carry

    def grow_moving(it):
        def body(col, carry):
            tile = moving[it, col // 4, lax.rem(col, 4)]
            for k in range(3):
                for c in range(3):
                    near_moving[col, k, c] = expanded(tile[c : c + 1], k)
            return carry

        lax.fori_loop(0, 16, body, 0)

    low = lax.broadcasted_iota(jnp.int32, (SIDE, 128), 0)
    cell_z = lax.broadcasted_iota(jnp.int32, (SIDE, 128), 1) // 8

    def weights(ex, ey):
        col = ex * 3 + ey
        tile = fixed[ex, ey]
        anchor = tile[0:3].astype(jnp.int32)
        value, slope = zip(*[spline(tile[c + 3 : c + 4]) for c in range(3)])
        place_x = low - (anchor[0:1] + (ex - 1) * 8)
        place_y = low - (anchor[1:2] + (ey - 1) * 8)
        place_z = low - anchor[2:3]
        wx, sx = placed(place_x, value[0]), placed(place_x, slope[0])
        wy, sy = placed(place_y, value[1]), placed(place_y, slope[1])
        for x in range(*SUPPORT[ex]):
            rows = pl.ds(x * SIDE, SIDE)
            prod[col, 0, rows] = sx[x : x + 1] * wy
            prod[col, 1, rows] = wx[x : x + 1] * sy
            prod[col, 2, rows] = wx[x : x + 1] * wy
        for k, source in enumerate((value[2], slope[2])):
            base = placed(place_z, source)
            spill = placed(place_z + SIDE, source)
            full = jnp.concatenate(
                [
                    jnp.where(
                        cell_z == cell,
                        base,
                        jnp.where(cell_z == (cell + SIDE - 1) % SIDE, spill, 0.0),
                    )
                    for cell in range(SIDE)
                ],
                axis=0,
            )
            lanes = pl.ds(pl.multiple_of(col * N + 128 * k, 128), 128)
            wz_hi[:, lanes], wz_lo[:, lanes] = halves(full)
            wt_hi[lanes, :], wt_lo[lanes, :] = halves(full.T)

    def weights_of(ex):
        def body(ey, carry):
            weights(ex, ey)
            return carry

        return body

    def spread_columns(it, groups, fresh):
        for ex, first, last in groups:
            rows = slice(SUPPORT[ex][0] * SIDE, SUPPORT[ex][1] * SIDE)
            for ey in range(first, last):
                col = 3 * ex + ey
                tile = moving[it, ex, ey]
                plain = tile[0:1] * prod[col, 0, rows] + tile[1:2] * prod[col, 1, rows]
                steep = tile[2:3] * prod[col, 2, rows]
                left = slice(col * N, col * N + 128)
                right = slice(col * N + 128, col * N + N)
                p_hi[rows, left], p_lo[rows, left] = halves(plain)
                p_hi[rows, right], p_lo[rows, right] = halves(steep)
            span = slice(N * (3 * ex + first), N * (3 * ex + last))
            term = product((p_hi[rows, span], p_lo[rows, span]), (wt_hi[span], wt_lo[span]))
            if fresh and ex == 1:
                spread[rows] = term
                spread[rows.stop :] = jnp.zeros((N - rows.stop, N), F32)
            else:
                spread[rows] += term

    def first_moment(ex, ey):
        tile = fixed[ex, ey]
        moving[0, ex, ey] = tile[7:8] * tile[8:16]

    owned = [(ex, ey) for ex in (1, 2) for ey in (1, 2)]
    for ex, ey in owned:
        first_moment(ex, ey)
    lax.fori_loop(1, 3, weights_of(1), 0)
    lax.fori_loop(1, 3, weights_of(2), 0)
    spread_columns(0, ((1, 1, 3), (2, 1, 3)), True)
    for copy in first_halo:
        copy.wait()
    for ex in range(4):
        for ey in range(4):
            if (ex, ey) not in owned:
                first_moment(ex, ey)
    for ey in range(3):
        weights(0, ey)
    weights(1, 0)
    weights(2, 0)
    spread_columns(0, ((1, 0, 1), (2, 0, 1), (0, 0, 3)), False)

    def pairs(item, carry):
        q = item // 9
        nb = lax.rem(item, 9)
        cx = q // 2
        cy = lax.rem(q, 2)
        dx = nb // 3 - 1
        dy = lax.rem(nb, 3) - 1
        tile = fixed[cx + 1, cy + 1]
        here = [tile[c : c + 1] + 1.0 + tile[c + 3 : c + 4] for c in range(3)]
        here[0] = here[0] - (8 * dx).astype(F32)
        here[1] = here[1] - (8 * dy).astype(F32)
        mine = tile[6:7]
        col = (cx + 1 + dx) * 4 + cy + 1 + dy
        for k in range(3):
            apart = [here[c] - near_static[col, k, c] for c in range(3)]
            square = apart[0] * apart[0] + apart[1] * apart[1] + apart[2] * apart[2]
            root = lax.rsqrt(mine * near_static[col, k, 3])
            if k == 1:
                same = (row == lane % 8) & (nb == 4)
                square = jnp.where(same, 1.0, square)
            c1, c2 = pair_coefficients(square, root)
            if k == 1:
                c1 = jnp.where(same, 0.0, c1)
                c2 = jnp.where(same, 0.0, c2)
            scaled = [c2 * apart[c] for c in range(3)]
            tensor[item, k, 0] = scaled[0] * apart[0] - c1
            tensor[item, k, 1] = scaled[1] * apart[1] - c1
            tensor[item, k, 2] = scaled[2] * apart[2] - c1
            tensor[item, k, 3] = scaled[0] * apart[1]
            tensor[item, k, 4] = scaled[0] * apart[2]
            tensor[item, k, 5] = scaled[1] * apart[2]
        return carry

    def near_field(it):
        grow_moving(it)

        def body(q, carry):
            cx = q // 2
            cy = lax.rem(q, 2)

            def inner(nb, total):
                fx, fy, fz = total
                col = (cx + nb // 3) * 4 + cy + lax.rem(nb, 3)
                item = q * 9 + nb
                for k in range(3):
                    vx, vy, vz = [near_moving[col, k, c] for c in range(3)]
                    xx, yy, zz, xy, xz, yz = [tensor[item, k, c] for c in range(6)]
                    fx = fx + (xx * vx + xy * vy + xz * vz)
                    fy = fy + (xy * vx + yy * vy + yz * vz)
                    fz = fz + (xz * vx + yz * vy + zz * vz)
                return fx, fy, fz

            zero = jnp.zeros((8, 128), F32)
            sums = lax.fori_loop(0, 9, inner, (zero, zero, zero))
            near[q] = jnp.concatenate(
                [jnp.sum(s, axis=0, keepdims=True) for s in sums]
                + [jnp.zeros((5, 128), F32)],
                axis=0,
            )
            return carry

        lax.fori_loop(0, 4, body, 0)

    def exchange(source, target, k):
        for route in ROUTES:
            gx, gy = place(*route)
            pltpu.make_async_remote_copy(
                src_ref=source.at[gx * SIDE + gy],
                dst_ref=target.at[me],
                send_sem=send_s.at[k],
                recv_sem=recv_s.at[k],
                device_id=(gx, gy),
                device_id_type=MESH,
            ).start()

        target[me] = source[me]

    def arrive(source, target, k):
        pltpu.make_async_remote_copy(
            src_ref=source.at[pl.ds(0, N - 1)],
            dst_ref=target.at[pl.ds(0, N - 1)],
            send_sem=send_s.at[k],
            recv_sem=recv_s.at[k],
            device_id=(mx, wrap(my + 1)),
            device_id_type=MESH,
        ).wait()

    def wave(k):
        return waves[0, N * k : N * (k + 1)], waves[1, N * k : N * (k + 1)]

    def put_rows(ref, value):
        ref[:, 0, :] = value[:, :128]
        ref[:, 1, :] = value[:, 128:]

    def get_rows(ref):
        return jnp.concatenate([ref[:, 0, :], ref[:, 1, :]], axis=1)

    def fill_green():
        line = jnp.zeros((1, 128), F32) + me.astype(F32)
        signed = jnp.where(line < N // 2, line, line - N) * (1.0 / N)
        height = signed * signed
        bend = 2.0 + jnp.cos(line * (2.0 * math.pi / N))
        strength = jnp.exp(-((math.pi / BETA) ** 2) * height) * 9.0 / (bend * bend)
        height = jnp.concatenate([height, height], axis=1)
        strength = jnp.concatenate([strength, strength], axis=1)
        square = plane[3] + height
        centre = square == 0.0
        plane[2] = jnp.where(
            centre, 0.0, plane[2] * strength / jnp.where(centre, 1.0, square)
        )

    def filtered(value):
        cosine = wave(1)
        sine = wave(2)
        upper = tuple(
            jnp.concatenate([c[:HALF], s[:HALF]], axis=0) for c, s in zip(cosine, sine)
        )
        both = product(upper, halves(value))
        re, im = both[:HALF], both[HALF:]
        tr, ti = plane[0], plane[1]
        both = halves(jnp.concatenate([re * tr - im * ti, re * ti + im * tr], axis=0))
        by_cosine = product(both, cosine)
        by_sine = product(both, sine)
        re = by_cosine[:HALF] - by_sine[HALF:]
        im = by_sine[:HALF] + by_cosine[HALF:]
        green = plane[2]
        both = halves(jnp.concatenate([re * green, im * green], axis=0))
        by_cosine = product(both, cosine)
        by_sine = product(both, sine)
        re = by_cosine[:HALF] + by_sine[HALF:]
        im = by_cosine[HALF:] - by_sine[:HALF]
        first = halves(re * tr + im * ti)
        other = halves(im * tr - re * ti)
        cosine = tuple(c[:, :HALF] for c in cosine)
        sine = tuple(c[:, :HALF] for c in sine)
        return product(cosine, first) + product(sine, other)

    def iteration(it, carry):
        @pl.when(it > 0)
        def _():
            spread_columns(it, ((1, 0, 3), (2, 0, 3), (0, 0, 3)), True)

        @pl.when(it == 0)
        def _():
            for copy in table_copies:
                copy.wait()

        put_rows(send_a, product(wave(0), halves(spread[...]), NT))

        @pl.when(it == 0)
        def _():
            pl.semaphore_wait(second_level, len(line_peers))

        exchange(send_a, land_a.at[it], 2 * it)

        @pl.when(it == 0)
        def _():
            lax.fori_loop(0, 16, grow_static, 0)
            lax.fori_loop(0, 36, pairs, 0)
            fill_green()

        arrive(send_a, land_a.at[it], 2 * it)
        put_rows(send_b, filtered(get_rows(land_a.at[it])))
        exchange(send_b, land_b.at[it], 2 * it + 1)
        near_field(it)

        @pl.when(it == 0)
        def _():
            def fold(col, carry):
                lanes = pl.ds(pl.multiple_of(col * N, N), N)
                wz_hi[:, lanes], wz_lo[:, lanes] = halves(
                    product(wave(0), (wz_hi[:, lanes], wz_lo[:, lanes]))
                )
                return carry

            lax.fori_loop(0, 9, fold, 0)

        arrive(send_b, land_b.at[it], 2 * it + 1)
        turned = halves(get_rows(land_b.at[it]).T)

        def gather(col):
            lanes = slice(col * N, col * N + N)
            ex, ey = col // 3, col % 3
            rows = slice(SUPPORT[ex][0] * SIDE, SUPPORT[ex][1] * SIDE)
            sampled = product(
                tuple(t[rows] for t in turned), (wz_hi[:, lanes], wz_lo[:, lanes])
            )
            plain = sampled[:, :128]
            steep = sampled[:, 128:]
            total = jnp.concatenate(
                [
                    -jnp.sum(prod[col, 0, rows] * plain, axis=0, keepdims=True),
                    -jnp.sum(prod[col, 1, rows] * plain, axis=0, keepdims=True),
                    -jnp.sum(prod[col, 2, rows] * steep, axis=0, keepdims=True),
                    jnp.zeros((5, 128), F32),
                ],
                axis=0,
            )
            if ex >= 1 and ey >= 1:
                total = total + near[2 * ex + ey - 3] + SELF_GAIN * moving[it, ex, ey]
            part[ex, ey] = total

        for col in (0, 1, 2, 3, 6):
            gather(col)

        def last_copies():
            copies = []
            for k, (a, b) in enumerate(((1, 0), (0, 1), (1, 1))):
                span = {0: (1, 2), 1: (0, 1)}
                land = {0: (0, 2), 1: (0, 1)}
                copies.append(
                    pltpu.make_async_remote_copy(
                        src_ref=part.at[spans(span, a, b)],
                        dst_ref=last_in.at[(k, *spans(land, a, b))],
                        send_sem=part_send.at[k],
                        recv_sem=part_recv.at[k],
                        device_id=(wrap(mx - a), wrap(my - b)),
                        device_id_type=MESH,
                    )
                )
            return copies

        @pl.when(it == ITERS - 1)
        def _():
            for copy in last_copies():
                copy.start()

        for col in (4, 5, 7, 8):
            gather(col)

        @pl.when(it == 0)
        def _():
            copies = part_copies()
            for copy in copies:
                copy.start()
            for copy in copies:
                copy.wait()
            reach = {0: ((-1, 0), (0, 0)), 1: ((0, 1),), 2: ((0, 2), (1, 0)), 3: ((1, 1),)}
            for ex in range(4):
                for ey in range(4):
                    total = jnp.zeros((8, 128), F32)
                    for a, i in reach[ex]:
                        for b, j in reach[ey]:
                            if a == 0 and b == 0:
                                total = total + part[i, j]
                            else:
                                total = total + inbox[sides.index((a, b)), i, j]
                    moving[1, ex, ey] = fixed[ex, ey, 7:8] * (fixed[ex, ey, 8:16] + total)

        @pl.when(it == ITERS - 1)
        def _():
            for copy in last_copies():
                copy.wait()
            for cx in range(2):
                for cy in range(2):
                    total = part[cx + 1, cy + 1]
                    if cx == 1:
                        total = total + last_in[0, 0, cy]
                    if cy == 1:
                        total = total + last_in[1, cx, 0]
                    if cx == 1 and cy == 1:
                        total = total + last_in[2, 0, 0]
                    tile = fixed[cx + 1, cy + 1]
                    result = tile[7:8] * (tile[8:16] + total)
                    for c in range(3):
                        out[c, cx, cy : cy + 1] = result[c : c + 1]

        return carry

    lax.fori_loop(0, ITERS, iteration, 0)


def shards(cotangent, polarizability, site_offset, site_fraction, cell_count):
    vmem = pl.BlockSpec(memory_space=pltpu.VMEM)

    def room(*shape, dtype=F32):
        return pltpu.VMEM(shape, dtype)

    dma = pltpu.SemaphoreType.DMA
    return pl.pallas_call(
        kernel,
        out_shape=jax.ShapeDtypeStruct((3, 2, 2, 128), F32),
        in_specs=[pl.BlockSpec(memory_space=pl.ANY)] * 7,
        out_specs=vmem,
        scratch_shapes=[
            room(3, 2, 2, 128),
            room(2, 2, 128),
            room(3, 2, 2, 128, dtype=jnp.int32),
            room(3, 2, 2, 128),
            room(2, 2, 16, dtype=jnp.int32),
            room(2, 3 * N, N, dtype=BF16),
            room(4, HALF, N),
            room(4, 4, 16, 128),
            room(2, 4, 4, 8, 128),
            room(9, 3, N, 128),
            room(N, 9 * N, dtype=BF16),
            room(N, 9 * N, dtype=BF16),
            room(9 * N, N, dtype=BF16),
            room(9 * N, N, dtype=BF16),
            room(N, 9 * N, dtype=BF16),
            room(N, 9 * N, dtype=BF16),
            room(N, N),
            room(N, 2, 128),
            room(N, 2, 128),
            room(2, N, 2, 128),
            room(2, N, 2, 128),
            room(16, 3, 4, 8, 128),
            room(16, 3, 3, 8, 128),
            room(36, 3, 6, 8, 128),
            room(4, 8, 128),
            room(3, 3, 8, 128),
            room(8, 3, 3, 8, 128),
            room(3, 2, 2, 8, 128),
            dma((7,)),
            dma((4,)),
            dma((4,)),
            dma((2, 8)),
            dma((2, 8)),
            dma((3,)),
            dma((3,)),
            pltpu.SemaphoreType.REGULAR,
        ],
        compiler_params=pltpu.CompilerParams(
            collective_id=0, has_side_effects=True, vmem_limit_bytes=56 * 1024 * 1024
        ),
    )(
        cotangent,
        polarizability,
        site_offset,
        site_fraction,
        cell_count,
        *[jnp.asarray(table) for table in TABLES],
    )


def solution(mesh):
    return jax.shard_map(
        shards,
        mesh=mesh,
        in_specs=(
            P(None, "gx", "gy", None),
            P("gx", "gy", None),
            P(None, "gx", "gy", None),
            P(None, "gx", "gy", None),
            P("gx", "gy", None),
        ),
        out_specs=P(None, "gx", "gy", None),
        check_vma=False,
    )
```
